256 devices in a mesh: row: 16 (over z_lo, x, core), col: 16 (over y, z_hi).
Axes of the slice: x: 4, y: 4, z: 8 (z_hi: 4, z_lo: 2; z = z_hi * 2 + z_lo), core: 2. Of those that a mesh axis runs over, the one named last changes fastest.
Arguments:
- inputs: bfloat16 [2048, 8192], P('col', 'row'), may hold values from -6 to 6
- cotangent: bfloat16 [2048, 8192], P('col', 'row'), may hold values from -6 to 6
- gate_pre: bfloat16 [2048, 16384], P('row', 'col'), may hold values from -8 to 8
- up_pre: bfloat16 [2048, 16384], P('row', 'col'), may hold values from -6 to 6
- w_gate: bfloat16 [8192, 16384], P('row', 'col'), may hold values from -0.0625 to 0.0625
- w_up: bfloat16 [8192, 16384], P('row', 'col'), may hold values from -0.0625 to 0.0625
- w_down: bfloat16 [16384, 8192], P('col', 'row'), may hold values from -0.046875 to 0.046875
Outputs:
- grad_inputs: bfloat16 [2048, 8192], P('col', 'row')
- grad_gate: float32 [8192, 16384], P('row', 'col')
- grad_up: float32 [8192, 16384], P('row', 'col')
- grad_down: float32 [16384, 8192], P('col', 'row')
The draws below stay inside these ranges and needn't reach their ends.
All inputs are finite; a program needn't handle non-finite values.
Results may differ from the reference program's by a relative error of at most 0.0049.
Values may be sent and summed in bfloat16 or wider, within the bound.
A program may use at most 128 MiB of HBM per device.

```python
import math
import jax
import jax.numpy as jnp

D = 8192
FF = 16384
TOKENS = 2048


def block_scale(own_key, extent, shards, smallest, largest):
    gain = 1.0
    for axis_at, parts in shards:
        draws = jax.random.uniform(jax.random.fold_in(jax.random.fold_in(own_key, 6), axis_at), (parts,), jnp.float32, smallest / len(shards), largest / len(shards))
        gain = gain * jnp.repeat(jnp.exp(draws), extent[axis_at] // parts).reshape((-1,) + (1,) * (len(extent) - 1 - axis_at))
    return gain


def normal_values(own_key, dims, spread, most, cuts=(), kind=jnp.bfloat16):
    level = block_scale(own_key, dims, cuts, -0.22, 0.18) if cuts else 1.0
    entries = jax.random.normal(own_key, dims, jnp.float32) * spread * level
    return jnp.minimum(jnp.maximum(entries, -most), most).astype(kind)


def setup_inputs(seed: int = 0) -> dict:
    splits = jax.random.split(jax.random.key(seed), 8)
    return {
        "inputs": normal_values(splits[0], (TOKENS, D), 1.0, 6.0, ((0, 16), (1, 16))),
        "cotangent": normal_values(splits[1], (TOKENS, D), 1.0, 6.0, ((0, 16), (1, 16))),
        "gate_pre": normal_values(splits[2], (TOKENS, FF), 1.5, 8.0, ((0, 16), (1, 16))),
        "up_pre": normal_values(splits[3], (TOKENS, FF), 1.0, 6.0, ((0, 16), (1, 16))),
        "w_gate": normal_values(splits[4], (D, FF), D ** -0.5, 0.0625, ((0, 16), (1, 16))),
        "w_up": normal_values(splits[5], (D, FF), D ** -0.5, 0.0625, ((0, 16), (1, 16))),
        "w_down": normal_values(splits[6], (FF, D), FF ** -0.5, 0.046875, ((0, 16), (1, 16))),
    }


def reference(inputs, cotangent, gate_pre, up_pre, w_gate, w_up, w_down):
    gate_f = gate_pre.astype(jnp.float32)
    up_f = up_pre.astype(jnp.float32)
    sig = jax.nn.sigmoid(gate_f)
    act = gate_f * sig
    hidden = (act * up_f).astype(jnp.bfloat16)
    grad_hidden = jnp.dot(cotangent, w_down.T, preferred_element_type=jnp.float32)
    grad_gate_pre = (grad_hidden * up_f * sig * (1.0 + gate_f * (1.0 - sig))).astype(jnp.bfloat16)
    grad_up_pre = (grad_hidden * act).astype(jnp.bfloat16)
    grad_inputs = jnp.dot(grad_gate_pre, w_gate.T, preferred_element_type=jnp.float32)
    grad_inputs = grad_inputs + jnp.dot(grad_up_pre, w_up.T, preferred_element_type=jnp.float32)
    scale = 1.0 / math.sqrt(inputs.shape[0])
    grad_gate = jnp.dot(inputs.T, grad_gate_pre, preferred_element_type=jnp.float32) * scale
    grad_up = jnp.dot(inputs.T, grad_up_pre, preferred_element_type=jnp.float32) * scale
    grad_down = jnp.dot(hidden.T, cotangent, preferred_element_type=jnp.float32) * scale
    return (grad_inputs.astype(jnp.bfloat16), grad_gate, grad_up, grad_down)
```

```python
import functools
import math

import jax
import jax.numpy as jnp
from jax import lax
from jax.experimental import pallas as pl
from jax.experimental.pallas import tpu as pltpu
from jax.sharding import Mesh
from jax.sharding import PartitionSpec as P

ROW = ("zl", "x", "core")
COL = ("y", "zh")
SIZES = {"zl": 2, "x": 4, "core": 2, "y": 4, "zh": 4}
MESH = pl.DeviceIdType.MESH
F32, BF16 = jnp.float32, jnp.bfloat16
NH = 2
N_SEM = 200


def nt(left, right):
    return lax.dot_general(left, right, (((1,), (1,)), ((), ())), preferred_element_type=F32)


def kernel(
    scale,
    inp_hbm, cot_hbm, gate_hbm, up_hbm, wg_hbm, wu_hbm, wd_hbm,
    gi_hbm, gg_hbm, gup_hbm, gd_hbm,
    CT, IN, INT, HID, GU, WD, WGU, GATE, UP,
    PC, RC, S, XA, XAR, XB, XBR, R, ZS, ZR,
    GIP, YA, YAR, YB, YBR, R2, HA, HAR, HB, HBR,
    OG, OD, OGI,
    ssem, rsem, lsem,
):
    at = {a: lax.axis_index(a) for a in SIZES}
    x, y, zh, zl, k = at["x"], at["y"], at["zh"], at["zl"], at["core"]
    br = CT.shape[3]

    def step(axis, d):
        return lax.rem(at[axis] + (d + SIZES[axis]), SIZES[axis])

    def peer(axis, d):
        return {axis: step(axis, d)}

    sends = []

    def send(src, dst, to):
        i = len(sends)
        c = pltpu.make_async_remote_copy(
            src_ref=src, dst_ref=dst, send_sem=ssem.at[i], recv_sem=rsem.at[i],
            device_id=to, device_id_type=MESH,
        )
        c.start()
        sends.append(c)
        return c

    n_local = [0]

    def local(src, dst):
        c = pltpu.make_async_copy(src, dst, lsem.at[n_local[0]])
        n_local[0] += 1
        c.start()
        return c

    ck, cb = lax.rem(zh, 2), 2 * y + zh // 2

    own_cot = local(cot_hbm, CT.at[:, ck, cb])
    load_gate = local(gate_hbm, GATE)
    load_up = local(up_hbm, UP)
    load_wd = local(wd_hbm, WD)
    own_inp = local(inp_hbm, IN.at[:, ck, cb])
    load_wg = local(wg_hbm, WGU.at[:, pl.ds(0, 1024)])
    load_wu = local(wu_hbm, WGU.at[:, pl.ds(1024, 1024)])

    barrier = pltpu.get_barrier_semaphore()
    peers = [peer("x", 1), peer("x", -1), peer("y", 1), peer("y", -1), peer("zh", 1), peer("zh", -1),
             peer("zl", 1), peer("core", 1)]
    for p in peers:
        pl.semaphore_signal(barrier, inc=1, device_id=p, device_id_type=MESH)
    pl.semaphore_wait(barrier, len(peers))

    class ColGather:
        def __init__(self, block, halves):
            self.block, self.halves = block, halves
            self.ys = {}
            self.fwd = []

        def at(self, dy, dz):
            yy, zz = step("y", dy), step("zh", dz)
            return self.block(lax.rem(zz, 2), 2 * yy + zz // 2)

        def ysend(self, dz):
            b = self.at(0, dz)
            self.ys[dz] = (send(b, b, peer("y", 1)), send(b, b, peer("y", -1)))

        def start(self):
            b = self.at(0, 0)
            self.z1 = (send(b, b, peer("zh", 1)), send(b, b, peer("zh", -1)))
            self.ysend(0)

        def zfwd(self):
            self.z1[0].wait_recv()
            b = self.halves(self.at(0, -1))[0]
            first = send(b, b, peer("zh", 1))
            self.z1[1].wait_recv()
            b = self.halves(self.at(0, 1))[1]
            second = send(b, b, peer("zh", -1))
            self.z2 = (first, second)

        def zlast(self):
            self.z2[0].wait_recv()
            self.z2[1].wait_recv()
            self.ysend(2)

        def yfwd(self, dz):
            up, down = self.ys[dz]
            up.wait_recv()
            if dz in (0, 2):
                b = self.at(-1, dz)
                self.fwd.append(send(b, b, peer("y", 1)))
            down.wait_recv()
            if dz in (1, -1):
                b = self.at(1, dz)
                self.fwd.append(send(b, b, peer("y", -1)))

        def finish(self):
            for c in self.fwd:
                c.wait_recv()

    def row_halves(ref):
        return ref.at[pl.ds(0, br // 2)], ref.at[pl.ds(br // 2, br // 2)]

    def piece_halves(ref):
        return ref.at[pl.ds(0, NH // 2)], ref.at[pl.ds(NH // 2, NH // 2)]

    cg = [ColGather(lambda q, b, h=h: CT.at[h, q, b], row_halves) for h in range(NH)]
    cgi = ColGather(lambda q, b: IN.at[:, q, b], piece_halves)

    class RowGather:
        def __init__(self, block):
            self.block = block
            self.core = []
            self.fwd = []
            self.xs = {}

        def at(self, dx, dzl):
            return self.block(k, step("zl", dzl) * 4 + step("x", dx))

        def share(self, dx, dzl):
            b = self.at(dx, dzl)
            self.core.append(send(b, b, peer("core", 1)))

        def xsend(self, dzl):
            b = self.at(0, dzl)
            self.xs[dzl] = (send(b, b, peer("x", 1)), send(b, b, peer("x", -1)))

        def start(self):
            b = self.at(0, 0)
            self.z = send(b, b, peer("zl", 1))
            self.xsend(0)
            self.share(0, 0)

        def zstep(self):
            self.z.wait_recv()
            self.xsend(1)
            self.share(0, 1)

        def xfwd(self, dzl):
            up, down = self.xs[dzl]
            up.wait_recv()
            b = self.at(-1, dzl)
            if dzl == 0:
                self.fwd.append(send(b, b, peer("x", 1)))
            self.share(-1, dzl)
            down.wait_recv()
            b = self.at(1, dzl)
            if dzl == 1:
                self.fwd.append(send(b, b, peer("x", -1)))
            self.share(1, dzl)

        def xlast(self):
            for dzl, c in enumerate(self.fwd):
                c.wait_recv()
                self.share(2, dzl)

        def finish(self):
            for c in self.core:
                c.wait_recv()

    hg = RowGather(lambda q, b: HID.at[:, q, b])
    rg = [RowGather(lambda q, b, h=h: GU.at[h, q, b]) for h in range(NH)]

    def hidden():
        load_gate.wait()
        load_up.wait()

        @pl.loop(0, NH * br // 32)
        def _(i):
            h, s = i // (br // 32), pl.multiple_of(lax.rem(i, br // 32) * 32, 32)
            g = GATE[h, pl.ds(s, 32)].astype(F32)
            u = UP[h, pl.ds(s, 32)].astype(F32)
            HID[h, k, zl * 4 + x, pl.ds(s, 32)] = (g * jax.nn.sigmoid(g) * u).astype(BF16)

    def gh_other(h):
        @pl.loop(0, 4)
        def _(n):
            c = pl.multiple_of(n * 256, 256)
            a = CT[h, 1 - k].reshape(8 * br, CT.shape[4])
            p = nt(a, WD[pl.ds(c, 256), :])
            PC[h, :, :, pl.ds(c, 256)] = p.astype(PC.dtype).reshape(8, br, 256)

        return send(PC.at[h], RC.at[h], peer("core", 1))

    def gh_own(h):
        @pl.loop(0, 4)
        def _(n):
            c = pl.multiple_of(n * 256, 256)
            a = CT[h, k].reshape(8 * br, CT.shape[4])
            S[h, :, :, pl.ds(c, 256)] = nt(a, WD[pl.ds(c, 256), :]).reshape(8, br, 256)

    class XScatter:
        def __init__(self, h):
            self.h = h

        def part(self, dx, z):
            return z * 4 + step("x", dx)

        def first(self, core):
            h = self.h
            core.wait_recv()

            def total(b):
                return S[h, b] + RC[h, b].astype(F32)

            for z in range(2):
                XA[h, z] = total(self.part(2, z)).astype(BF16)
            self.a = (send(XA.at[h, 0], XAR.at[h, 0], peer("x", 1)), send(XA.at[h, 1], XAR.at[h, 1], peer("x", -1)))
            XB[h, 0, 1] = total(self.part(1, 1)).astype(BF16)
            XB[h, 1, 0] = total(self.part(-1, 0)).astype(BF16)
            self.b1 = (send(XB.at[h, 0, 1], XBR.at[h, 0, 1], peer("x", 1)),
                       send(XB.at[h, 1, 0], XBR.at[h, 1, 0], peer("x", -1)))
            for b in (self.part(1, 0), self.part(-1, 1), self.part(0, 0), self.part(0, 1)):
                S[h, b] = total(b)

        def second(self):
            h = self.h
            self.a[0].wait_recv()
            XB[h, 0, 0] = (S[h, self.part(1, 0)] + XAR[h, 0].astype(F32)).astype(BF16)
            self.a[1].wait_recv()
            XB[h, 1, 1] = (S[h, self.part(-1, 1)] + XAR[h, 1].astype(F32)).astype(BF16)
            self.b2 = (send(XB.at[h, 0, 0], XBR.at[h, 0, 0], peer("x", 1)),
                       send(XB.at[h, 1, 1], XBR.at[h, 1, 1], peer("x", -1)))

        def third(self):
            h = self.h
            for c in self.b1 + self.b2:
                c.wait_recv()

            def total(z):
                return S[h, self.part(0, z)] + XBR[h, 0, z].astype(F32) + XBR[h, 1, z].astype(F32)

            ZS[h] = total(1 - zl).astype(ZS.dtype)
            self.z = send(ZS.at[h], ZR.at[h], peer("zl", 1))
            R[h] = total(zl)

        def grads(self):
            h = self.h
            self.z.wait_recv()

            @pl.loop(0, br // 16)
            def _(i):
                s = pl.multiple_of(i * 16, 16)
                gh = R[h, pl.ds(s, 16)] + ZR[h, pl.ds(s, 16)].astype(F32)
                g = GATE[h, pl.ds(s, 16)].astype(F32)
                u = UP[h, pl.ds(s, 16)].astype(F32)
                sig = jax.nn.sigmoid(g)
                b = zl * 4 + x
                GU[h, k, b, pl.ds(s, 16), pl.ds(0, 1024)] = (gh * u * sig * (1.0 + g * (1.0 - sig))).astype(BF16)
                GU[h, k, b, pl.ds(s, 16), pl.ds(1024, 1024)] = (gh * (g * sig)).astype(BF16)

    xs = [XScatter(h) for h in range(NH)]

    def gi(h):
        @pl.loop(0, 4)
        def _(i):
            q, c = i // 2, pl.multiple_of(lax.rem(i, 2) * 256, 256)
            a = GU[h, q].reshape(8 * br, GU.shape[4])
            GIP[h, q, :, :, pl.ds(c, 256)] = nt(a, WGU[pl.ds(c, 256), :]).reshape(8, br, 256)

    class YScatter:
        def __init__(self, h):
            self.h = h

        def part(self, dy, q):
            return GIP[self.h, q, pl.ds(2 * step("y", dy), 2)]

        def first(self):
            h = self.h
            for q in range(2):
                YA[h, q] = self.part(2, q).astype(BF16)
            self.a = (send(YA.at[h, 0], YAR.at[h, 0], peer("y", 1)), send(YA.at[h, 1], YAR.at[h, 1], peer("y", -1)))
            YB[h, 0, 1] = self.part(1, 1).astype(BF16)
            YB[h, 1, 0] = self.part(-1, 0).astype(BF16)
            self.b1 = (send(YB.at[h, 0, 1], YBR.at[h, 0, 1], peer("y", 1)),
                       send(YB.at[h, 1, 0], YBR.at[h, 1, 0], peer("y", -1)))

        def second(self):
            h = self.h
            self.a[0].wait_recv()
            YB[h, 0, 0] = (self.part(1, 0) + YAR[h, 0].astype(F32)).astype(BF16)
            self.a[1].wait_recv()
            YB[h, 1, 1] = (self.part(-1, 1) + YAR[h, 1].astype(F32)).astype(BF16)
            self.b2 = (send(YB.at[h, 0, 0], YBR.at[h, 0, 0], peer("y", 1)),
                       send(YB.at[h, 1, 1], YBR.at[h, 1, 1], peer("y", -1)))

        def third(self):
            h = self.h
            for c in self.b1 + self.b2:
                c.wait_recv()
            for q in range(2):
                R2[h, q] = self.part(0, q) + YBR[h, 0, q].astype(F32) + YBR[h, 1, q].astype(F32)

            def zpart(dz, half):
                zz = step("zh", dz)
                return R2[h, lax.rem(zz, 2), zz // 2, pl.ds(half * (br // 2), br // 2)]

            self.zpart = zpart
            for half in range(2):
                HA[h, half] = zpart(2, half).astype(BF16)
            self.za = (send(HA.at[h, 0], HAR.at[h, 0], peer("zh", 1)), send(HA.at[h, 1], HAR.at[h, 1], peer("zh", -1)))
            HB[h, 0, 1] = zpart(1, 1).astype(BF16)
            HB[h, 1, 0] = zpart(-1, 0).astype(BF16)
            self.zb1 = (send(HB.at[h, 0, 1], HBR.at[h, 0, 1], peer("zh", 1)),
                        send(HB.at[h, 1, 0], HBR.at[h, 1, 0], peer("zh", -1)))

        def fourth(self):
            h = self.h
            self.za[0].wait_recv()
            HB[h, 0, 0] = (self.zpart(1, 0) + HAR[h, 0].astype(F32)).astype(BF16)
            self.za[1].wait_recv()
            HB[h, 1, 1] = (self.zpart(-1, 1) + HAR[h, 1].astype(F32)).astype(BF16)
            self.zb2 = (send(HB.at[h, 0, 0], HBR.at[h, 0, 0], peer("zh", 1)),
                        send(HB.at[h, 1, 1], HBR.at[h, 1, 1], peer("zh", -1)))

        def fifth(self):
            h = self.h
            for c in self.zb1 + self.zb2:
                c.wait_recv()
            for half in range(2):
                OGI[h, pl.ds(half * (br // 2), br // 2)] = (
                    self.zpart(0, half) + HBR[h, 0, half].astype(F32) + HBR[h, 1, half].astype(F32)
                ).astype(BF16)

    ysc = [YScatter(h) for h in range(NH)]

    def transpose_inputs():
        @pl.loop(0, NH * 2)
        def _(i):
            rows = 8 * br
            v = IN[i // 2, lax.rem(i, 2)].reshape(rows, IN.shape[4])
            INT[:, pl.ds(pl.multiple_of(i * rows, rows), rows)] = v.T

    def grad_down():
        @pl.loop(0, 4)
        def _(i):
            c = pl.multiple_of(i * 256, 256)
            a = HID[:, :, :, :, pl.ds(c, 256)].reshape(NH * 16 * br, 256)
            b = CT[...].reshape(NH * 16 * br, CT.shape[4])
            p = lax.dot_general(a, b, (((0,), (0,)), ((), ())), preferred_element_type=F32)
            OD[pl.ds(c, 256), :] = p * scale

    def grad_gu(h):
        rows = 16 * br

        @pl.loop(0, 8)
        def _(i):
            c = pl.multiple_of(i * 256, 256)
            p = jnp.dot(INT[:, pl.ds(h * rows, rows)], GU[h, :, :, :, pl.ds(c, 256)].reshape(rows, 256),
                        preferred_element_type=F32)
            if h > 0:
                p = p + OG[:, pl.ds(c, 256)]
            OG[:, pl.ds(c, 256)] = p * scale if h == NH - 1 else p

    own_cot.wait()
    for h in range(NH):
        cg[h].start()
    hidden()
    hg.start()
    load_wd.wait()
    cg[0].yfwd(0)
    cg[0].zfwd()
    cg[0].ysend(1)
    cg[0].ysend(-1)
    cg[1].yfwd(0)
    cg[1].zfwd()
    cg[0].zlast()
    own_inp.wait()
    cg[0].yfwd(1)
    cg[0].yfwd(-1)
    cg[1].ysend(1)
    cg[1].ysend(-1)
    hg.zstep()
    cg[0].yfwd(2)
    cg[1].zlast()
    cgi.start()
    hg.xfwd(0)
    cg[0].finish()
    core0 = gh_other(0)
    gh_own(0)
    cg[1].yfwd(1)
    cg[1].yfwd(-1)
    xs[0].first(core0)
    hg.xfwd(1)
    cg[1].yfwd(2)
    xs[0].second()
    cg[1].finish()
    core1 = gh_other(1)
    gh_own(1)
    xs[1].first(core1)
    cgi.zfwd()
    cgi.ysend(1)
    cgi.ysend(-1)
    xs[0].third()
    hg.xlast()
    xs[1].second()
    cgi.yfwd(0)
    xs[0].grads()
    rg[0].start()
    cgi.zlast()
    cgi.yfwd(1)
    cgi.yfwd(-1)
    rg[0].zstep()
    xs[1].third()
    load_wg.wait()
    load_wu.wait()
    hg.finish()
    cgi.yfwd(2)
    xs[1].grads()
    rg[1].start()
    rg[0].xfwd(0)
    rg[1].zstep()
    rg[0].xfwd(1)
    cgi.finish()
    transpose_inputs()
    rg[0].xlast()
    rg[0].finish()
    gi(0)
    ysc[0].first()
    rg[1].xfwd(0)
    ysc[0].second()
    rg[1].xfwd(1)
    grad_down()
    out_down = local(OD, gd_hbm)
    ysc[0].third()
    rg[1].xlast()
    ysc[0].fourth()
    grad_gu(0)
    rg[1].finish()
    gi(1)
    ysc[1].first()
    ysc[0].fifth()
    ysc[1].second()
    grad_gu(1)
    out_gate = local(OG.at[:, pl.ds(0, 1024)], gg_hbm)
    out_up = local(OG.at[:, pl.ds(1024, 1024)], gup_hbm)
    ysc[1].third()
    ysc[1].fourth()
    ysc[1].fifth()
    out_in = local(OGI, gi_hbm)
    for c in sends:
        c.wait_send()
    for c in (out_down, out_gate, out_up, out_in):
        c.wait()


def per_device(inputs, cotangent, gate_pre, up_pre, w_gate, w_up, w_down):
    t, d = inputs.shape
    ff = gate_pre.shape[1]
    br = t // NH
    tokens = 16 * t
    scale = 1.0 / math.sqrt(tokens)

    def vm(*shape, kind=BF16):
        return pltpu.VMEM(shape, kind)

    scratch = [
        vm(NH, 2, 8, br, d), vm(NH, 2, 8, br, d), vm(d, tokens), vm(NH, 2, 8, br, ff), vm(NH, 2, 8, br, 2 * ff),
        vm(ff, d), vm(d, 2 * ff), vm(NH, br, ff), vm(NH, br, ff),
        vm(NH, 8, br, ff), vm(NH, 8, br, ff), vm(NH, 8, br, ff, kind=F32),
        vm(NH, 2, br, ff), vm(NH, 2, br, ff), vm(NH, 2, 2, br, ff), vm(NH, 2, 2, br, ff),
        vm(NH, br, ff, kind=F32), vm(NH, br, ff), vm(NH, br, ff),
        vm(NH, 2, 8, br, d, kind=F32),
        vm(NH, 2, 2, br, d), vm(NH, 2, 2, br, d), vm(NH, 2, 2, 2, br, d), vm(NH, 2, 2, 2, br, d),
        vm(NH, 2, 2, br, d, kind=F32),
        vm(NH, 2, br // 2, d), vm(NH, 2, br // 2, d), vm(NH, 2, 2, br // 2, d), vm(NH, 2, 2, br // 2, d),
        vm(d, 2 * ff, kind=F32), vm(ff, d, kind=F32), vm(NH, br, d),
        pltpu.SemaphoreType.DMA((N_SEM,)), pltpu.SemaphoreType.DMA((N_SEM,)), pltpu.SemaphoreType.DMA((16,)),
    ]
    hbm = pl.BlockSpec(memory_space=pl.ANY)
    gi, gg, gup, gd = pl.pallas_call(
        functools.partial(kernel, scale),
        out_shape=(
            jax.ShapeDtypeStruct((NH, br, d), BF16),
            jax.ShapeDtypeStruct((d, ff), F32),
            jax.ShapeDtypeStruct((d, ff), F32),
            jax.ShapeDtypeStruct((ff, d), F32),
        ),
        in_specs=[hbm] * 7,
        out_specs=(hbm,) * 4,
        scratch_shapes=scratch,
        compiler_params=pltpu.CompilerParams(
            collective_id=0, has_side_effects=True, vmem_limit_bytes=63 * 1024 * 1024
        ),
    )(
        inputs.reshape(NH, br, d), cotangent.reshape(NH, br, d), gate_pre.reshape(NH, br, ff),
        up_pre.reshape(NH, br, ff), w_gate, w_up, w_down,
    )
    return gi.reshape(t, d), gg, gup, gd


def solution(mesh):
    split = Mesh(mesh.devices.reshape(2, 4, 2, 4, 4), ROW + COL)
    in_specs = (P(COL, ROW), P(COL, ROW), P(ROW, COL), P(ROW, COL), P(ROW, COL), P(ROW, COL), P(COL, ROW))
    out_specs = (P(COL, ROW), P(ROW, COL), P(ROW, COL), P(COL, ROW))
    return jax.shard_map(per_device, mesh=split, in_specs=in_specs, out_specs=out_specs, check_vma=False)
```

```python
import functools
import math

import jax
import jax.numpy as jnp
from jax import lax
from jax.experimental import pallas as pl
from jax.experimental.pallas import tpu as pltpu
from jax.sharding import Mesh
from jax.sharding import PartitionSpec as P

ROW = ("zl", "x", "core")
COL = ("y", "zh")
SIZES = {"zl": 2, "x": 4, "core": 2, "y": 4, "zh": 4}
MESH = pl.DeviceIdType.MESH
F32, BF16 = jnp.float32, jnp.bfloat16
NH = 4
RG_MODE = ('A', 'A', 'A', 'A')
HG_MODE = '0'
N_SEM = 320
VMEM_LIMIT = 50 * 1024 * 1024
TN = 512


def nt(left, right):
    return lax.dot_general(left, right, (((1,), (1,)), ((), ())), preferred_element_type=F32)


def kernel(
    scale,
    inp_hbm, cot_hbm, gate_hbm, up_hbm, wg_hbm, wu_hbm, wd_hbm,
    OGI, OGG, OGU, OD,
    CT, IN, INT, HID, GU, WD, WGU, GATE, UP,
    PC, RC, S, XA, XAR, XB, XBR, R, ZS, ZR,
    GIP, YA, YAR, YB, YBR, R2, HA, HAR, HB, HBR,
    ssem, rsem, lsem,
):
    at = {a: lax.axis_index(a) for a in SIZES}
    x, y, zh, zl, k = at["x"], at["y"], at["zh"], at["zl"], at["core"]
    br = CT.shape[3]

    def step(axis, d):
        return lax.rem(at[axis] + (d + SIZES[axis]), SIZES[axis])

    def peer(axis, d):
        return {axis: step(axis, d)}

    sends = []

    def send(src, dst, to):
        i = len(sends)
        c = pltpu.make_async_remote_copy(
            src_ref=src, dst_ref=dst, send_sem=ssem.at[i], recv_sem=rsem.at[i],
            device_id=to, device_id_type=MESH,
        )
        c.start()
        sends.append(c)
        return c

    n_local = [0]

    def local(src, dst):
        c = pltpu.make_async_copy(src, dst, lsem.at[n_local[0]])
        n_local[0] += 1
        c.start()
        return c

    ck, cb = lax.rem(zh, 2), 2 * y + zh // 2

    own_cot = local(cot_hbm, CT.at[:, ck, cb])
    load_gate = local(gate_hbm, GATE)
    load_up = local(up_hbm, UP)
    load_wd = local(wd_hbm, WD)
    own_inp = local(inp_hbm, IN.at[:, ck, cb])
    load_wg = local(wg_hbm, WGU.at[:, pl.ds(0, 1024)])
    load_wu = local(wu_hbm, WGU.at[:, pl.ds(1024, 1024)])

    barrier = pltpu.get_barrier_semaphore()
    peers = [peer("x", 1), peer("x", -1), peer("y", 1), peer("y", -1), peer("zh", 1), peer("zh", -1),
             peer("zl", 1), peer("core", 1)]
    for p in peers:
        pl.semaphore_signal(barrier, inc=1, device_id=p, device_id_type=MESH)
    pl.semaphore_wait(barrier, len(peers))

    class ColGather:
        def __init__(self, block, halves):
            self.block, self.halves = block, halves
            self.y, self.f = {}, {}

        def at(self, dy, dz):
            yy, zz = step("y", dy), step("zh", dz)
            return self.block(lax.rem(zz, 2), 2 * yy + zz // 2)

        def ysend(self, dz):
            b = self.at(0, dz)
            self.y[dz] = (send(b, b, peer("y", 1)), send(b, b, peer("y", -1)))

        def sz(self):
            b = self.at(0, 0)
            self.z1 = (send(b, b, peer("zh", 1)), send(b, b, peer("zh", -1)))

        def sy(self):
            self.ysend(0)

        def zfp(self):
            self.z1[0].wait_recv()
            b = self.halves(self.at(0, -1))[0]
            self.z2p = send(b, b, peer("zh", 1))

        def zfm(self):
            self.z1[1].wait_recv()
            b = self.halves(self.at(0, 1))[1]
            self.z2m = send(b, b, peer("zh", -1))

        def ys(self, dz):
            self.ysend(dz)

        def zl(self):
            self.z2p.wait_recv()
            self.z2m.wait_recv()
            self.ysend(2)

        def yfp(self, dz):
            self.y[dz][0].wait_recv()
            b = self.at(-1, dz)
            self.f[dz] = send(b, b, peer("y", 1))

        def yfm(self, dz):
            self.y[dz][1].wait_recv()
            b = self.at(1, dz)
            self.f[dz] = send(b, b, peer("y", -1))

        def fin(self):
            for dz in (0, 2):
                self.y[dz][1].wait_recv()
            for dz in (1, -1):
                self.y[dz][0].wait_recv()
            for c in self.f.values():
                c.wait_recv()

    def row_halves(ref):
        return ref.at[pl.ds(0, br // 2)], ref.at[pl.ds(br // 2, br // 2)]

    def piece_halves(ref):
        return ref.at[pl.ds(0, NH // 2)], ref.at[pl.ds(NH // 2, NH // 2)]

    cg = [ColGather(lambda q, b, h=h: CT.at[h, q, b], row_halves) for h in range(NH)]
    cgi = ColGather(lambda q, b: IN.at[:, q, b], piece_halves)

    class RowGather:
        def __init__(self, block, mode, mirror):
            self.block, self.mode, self.mirror = block, mode, mirror
            self.core = []

        def at(self, dx, dzl):
            return self.block(k, step("zl", dzl) * 4 + step("x", dx))

        def to(self, dx, dzl, axis, d=1):
            b = self.at(dx, dzl)
            return send(b, b, peer(axis, d))

        def share(self, dx, dzl):
            self.core.append(self.to(dx, dzl, "core"))

        def sz(self):
            self.z = self.to(0, 0, "zl")

        def sx(self):
            self.x0 = (self.to(0, 0, "x", 1), self.to(0, 0, "x", -1))

        def sc(self):
            self.share(0, 0)

        def f0p(self):
            self.x0[0].wait_recv()
            if not self.mirror:
                self.f0 = self.to(-1, 0, "x", 1)

        def s10(self):
            self.share(-1, 0)

        def f0m(self):
            self.x0[1].wait_recv()
            if self.mirror:
                self.f0 = self.to(1, 0, "x", -1)
            self.share(1, 0)

        def l0(self):
            self.f0.wait_recv()
            self.share(2, 0)

        def zx(self):
            self.z.wait_recv()
            up = self.to(0, 1, "x", 1) if self.mode != "B" else None
            self.x1 = (up, self.to(0, 1, "x", -1))

        def zc(self):
            self.share(0, 1)

        def zp(self):
            self.z1 = self.to(-1, 0, "zl")

        def z2(self):
            self.f1 = self.to(2, 0, "zl")

        def f1p(self):
            (self.z1 if self.mode == "B" else self.x1[0]).wait_recv()
            self.share(-1, 1)

        def f1m(self):
            self.x1[1].wait_recv()
            if self.mode == "0":
                self.f1 = self.to(1, 1, "x", -1)
            self.share(1, 1)

        def l1(self):
            self.f1.wait_recv()
            self.share(2, 1)

        def fin(self):
            for c in self.core:
                c.wait_recv()

    hg = RowGather(lambda q, b: HID.at[:, q, b], HG_MODE, False)
    rg = [RowGather(lambda q, b, h=h: GU.at[h, q, b], RG_MODE[h], RG_MODE[h] == "A" and h % 2 == 1) for h in range(NH)]

    ready = []

    def when(*copies):
        for c in copies:
            if id(c) not in ready:
                ready.append(id(c))
                c.wait()

    def hidden():
        when(load_gate, load_up)

        @pl.loop(0, NH * br // 32)
        def _(i):
            h, s = i // (br // 32), pl.multiple_of(lax.rem(i, br // 32) * 32, 32)
            g = GATE[h, pl.ds(s, 32)].astype(F32)
            u = UP[h, pl.ds(s, 32)].astype(F32)
            HID[h, k, zl * 4 + x, pl.ds(s, 32)] = (g * jax.nn.sigmoid(g) * u).astype(BF16)

    core_part = {}

    def gho(h):
        when(load_wd)

        @pl.loop(0, 1024 // TN)
        def _(n):
            c = pl.multiple_of(n * TN, TN)
            a = CT[h, 1 - k].reshape(8 * br, CT.shape[4])
            p = nt(a, WD[pl.ds(c, TN), :])
            PC[h, :, :, pl.ds(c, TN)] = p.astype(PC.dtype).reshape(8, br, TN)

        core_part[h] = send(PC.at[h], RC.at[h], peer("core", 1))

    def ghw(h):
        @pl.loop(0, 1024 // TN)
        def _(n):
            c = pl.multiple_of(n * TN, TN)
            a = CT[h, k].reshape(8 * br, CT.shape[4])
            S[h, :, :, pl.ds(c, TN)] = nt(a, WD[pl.ds(c, TN), :]).reshape(8, br, TN)

    class XScatter:
        def __init__(self, h):
            self.h = h

        def part(self, dx, z):
            return z * 4 + step("x", dx)

        def total(self, b):
            return S[self.h, b] + RC[self.h, b].astype(F32)

        def x1a(self):
            h = self.h
            core_part[h].wait_recv()
            for z in range(2):
                XA[h, z] = self.total(self.part(2, z)).astype(BF16)
            self.a = (send(XA.at[h, 0], XAR.at[h, 0], peer("x", 1)), send(XA.at[h, 1], XAR.at[h, 1], peer("x", -1)))

        def x1c(self):
            h = self.h
            XB[h, 0, 1] = self.total(self.part(1, 1)).astype(BF16)
            XB[h, 1, 0] = self.total(self.part(-1, 0)).astype(BF16)
            self.b1 = (send(XB.at[h, 0, 1], XBR.at[h, 0, 1], peer("x", 1)),
                       send(XB.at[h, 1, 0], XBR.at[h, 1, 0], peer("x", -1)))

        def x1b(self):
            for b in (self.part(1, 0), self.part(-1, 1), self.part(0, 0), self.part(0, 1)):
                S[self.h, b] = self.total(b)

        def x2p(self):
            h = self.h
            self.a[0].wait_recv()
            XB[h, 0, 0] = (S[h, self.part(1, 0)] + XAR[h, 0].astype(F32)).astype(BF16)
            self.b2p = send(XB.at[h, 0, 0], XBR.at[h, 0, 0], peer("x", 1))

        def x2m(self):
            h = self.h
            self.a[1].wait_recv()
            XB[h, 1, 1] = (S[h, self.part(-1, 1)] + XAR[h, 1].astype(F32)).astype(BF16)
            self.b2m = send(XB.at[h, 1, 1], XBR.at[h, 1, 1], peer("x", -1))

        def x3(self):
            h = self.h
            for c in self.b1 + (self.b2p, self.b2m):
                c.wait_recv()

            def total(z):
                return S[h, self.part(0, z)] + XBR[h, 0, z].astype(F32) + XBR[h, 1, z].astype(F32)

            ZS[h] = total(1 - zl).astype(ZS.dtype)
            self.z = send(ZS.at[h], ZR.at[h], peer("zl", 1))
            R[h] = total(zl)

        def grads(self):
            h = self.h
            self.z.wait_recv()

            @pl.loop(0, br // 16)
            def _(i):
                s = pl.multiple_of(i * 16, 16)
                gh = R[h, pl.ds(s, 16)] + ZR[h, pl.ds(s, 16)].astype(F32)
                g = GATE[h, pl.ds(s, 16)].astype(F32)
                u = UP[h, pl.ds(s, 16)].astype(F32)
                sig = jax.nn.sigmoid(g)
                b = zl * 4 + x
                GU[h, k, b, pl.ds(s, 16), pl.ds(0, 1024)] = (gh * u * sig * (1.0 + g * (1.0 - sig))).astype(BF16)
                GU[h, k, b, pl.ds(s, 16), pl.ds(1024, 1024)] = (gh * (g * sig)).astype(BF16)

    xs = [XScatter(h) for h in range(NH)]

    def gi(h):
        when(load_wg, load_wu)

        @pl.loop(0, 2)
        def _(q):
            @pl.loop(0, 512 // TN)
            def _(i):
                c = pl.multiple_of(i * TN, TN)
                a = GU[h, q].reshape(8 * br, GU.shape[4])
                GIP[h, q, :, :, pl.ds(c, TN)] = nt(a, WGU[pl.ds(c, TN), :]).reshape(8, br, TN)

    class YScatter:
        def __init__(self, h):
            self.h = h

        def part(self, dy, q):
            return GIP[self.h, q, pl.ds(2 * step("y", dy), 2)]

        def y1(self):
            h = self.h
            for q in range(2):
                YA[h, q] = self.part(2, q).astype(BF16)
            self.a = (send(YA.at[h, 0], YAR.at[h, 0], peer("y", 1)), send(YA.at[h, 1], YAR.at[h, 1], peer("y", -1)))

        def y1b(self):
            h = self.h
            YB[h, 0, 1] = self.part(1, 1).astype(BF16)
            YB[h, 1, 0] = self.part(-1, 0).astype(BF16)
            self.b1 = (send(YB.at[h, 0, 1], YBR.at[h, 0, 1], peer("y", 1)),
                       send(YB.at[h, 1, 0], YBR.at[h, 1, 0], peer("y", -1)))

        def y2p(self):
            h = self.h
            self.a[0].wait_recv()
            YB[h, 0, 0] = (self.part(1, 0) + YAR[h, 0].astype(F32)).astype(BF16)
            self.b2p = send(YB.at[h, 0, 0], YBR.at[h, 0, 0], peer("y", 1))

        def y2m(self):
            h = self.h
            self.a[1].wait_recv()
            YB[h, 1, 1] = (self.part(-1, 1) + YAR[h, 1].astype(F32)).astype(BF16)
            self.b2m = send(YB.at[h, 1, 1], YBR.at[h, 1, 1], peer("y", -1))

        def y3(self):
            h = self.h
            for c in self.b1 + (self.b2p, self.b2m):
                c.wait_recv()
            for q in range(2):
                R2[h, q] = self.part(0, q) + YBR[h, 0, q].astype(F32) + YBR[h, 1, q].astype(F32)

            def zpart(dz, half):
                zz = step("zh", dz)
                return R2[h, lax.rem(zz, 2), zz // 2, pl.ds(half * (br // 2), br // 2)]

            self.zpart = zpart
            for half in range(2):
                HA[h, half] = zpart(2, half).astype(BF16)
            self.za = (send(HA.at[h, 0], HAR.at[h, 0], peer("zh", 1)), send(HA.at[h, 1], HAR.at[h, 1], peer("zh", -1)))
            HB[h, 0, 1] = zpart(1, 1).astype(BF16)
            HB[h, 1, 0] = zpart(-1, 0).astype(BF16)
            self.zb1 = (send(HB.at[h, 0, 1], HBR.at[h, 0, 1], peer("zh", 1)),
                        send(HB.at[h, 1, 0], HBR.at[h, 1, 0], peer("zh", -1)))

        def y4p(self):
            h = self.h
            self.za[0].wait_recv()
            HB[h, 0, 0] = (self.zpart(1, 0) + HAR[h, 0].astype(F32)).astype(BF16)
            self.zb2p = send(HB.at[h, 0, 0], HBR.at[h, 0, 0], peer("zh", 1))

        def y4m(self):
            h = self.h
            self.za[1].wait_recv()
            HB[h, 1, 1] = (self.zpart(-1, 1) + HAR[h, 1].astype(F32)).astype(BF16)
            self.zb2m = send(HB.at[h, 1, 1], HBR.at[h, 1, 1], peer("zh", -1))

        def y5(self):
            h = self.h
            for c in self.zb1 + (self.zb2p, self.zb2m):
                c.wait_recv()
            for half in range(2):
                OGI[h, pl.ds(half * (br // 2), br // 2)] = (
                    self.zpart(0, half) + HBR[h, 0, half].astype(F32) + HBR[h, 1, half].astype(F32)
                ).astype(BF16)

    ys = [YScatter(h) for h in range(NH)]

    def transpose_inputs():
        @pl.loop(0, NH * 2)
        def _(i):
            rows = 8 * br
            v = IN[i // 2, lax.rem(i, 2)].reshape(rows, IN.shape[4])
            INT[:, pl.ds(pl.multiple_of(i * rows, rows), rows)] = v.T

    def grad_down():
        @pl.loop(0, 4)
        def _(i):
            c = pl.multiple_of(i * 256, 256)
            a = HID[:, :, :, :, pl.ds(c, 256)].reshape(NH * 16 * br, 256)
            b = CT[...].reshape(NH * 16 * br, CT.shape[4])
            p = lax.dot_general(a, b, (((0,), (0,)), ((), ())), preferred_element_type=F32)
            OD[pl.ds(c, 256), :] = p * scale

    added = []

    def gu(h):
        rows = 16 * br
        first, last = not added, len(added) == NH - 1
        added.append(h)

        for out, base in ((OGG, 0), (OGU, 1024)):
            @pl.loop(0, 4)
            def _(i):
                c = pl.multiple_of(i * 256, 256)
                from_gu = pl.ds(pl.multiple_of(base + i * 256, 256), 256)
                p = jnp.dot(INT[:, pl.ds(h * rows, rows)], GU[h, :, :, :, from_gu].reshape(rows, 256),
                            preferred_element_type=F32)
                if not first:
                    p = p + out[:, pl.ds(c, 256)]
                out[:, pl.ds(c, 256)] = p * scale if last else p

    own_cot.wait()
    own_inp.wait()
    cg[1].sz()
    cg[1].sy()
    hidden()
    hg.sx()
    cg[3].sy()
    cg[0].sz()
    cg[2].sy()
    cg[0].sy()
    cg[1].yfp(0)
    hg.sc()
    cg[3].yfp(0)
    cg[1].zfp()
    cg[1].ys(-1)
    cg[1].zfm()
    cg[1].ys(1)
    cg[0].zfm()
    cg[0].zfp()
    cg[0].ys(-1)
    cg[2].sz()
    cg[3].sz()
    cg[0].ys(1)
    cg[1].zl()
    cg[1].yfm(1)
    cg[2].yfp(0)
    hg.f0p()
    cg[0].zl()
    hg.s10()
    cg[1].yfm(-1)
    cg[1].yfp(2)
    cg[2].zfm()
    cg[2].ys(1)
    cg[0].yfm(1)
    cg[2].zfp()
    cg[0].yfm(-1)
    cgi.sz()
    cg[0].yfp(0)
    cg[0].yfp(2)
    cg[3].zfp()
    cg[3].ys(-1)
    cg[1].fin()
    hg.f0m()
    gho(1)
    cg[2].zl()
    ghw(1)
    xs[1].x1a()
    cg[0].fin()
    xs[1].x1c()
    xs[1].x1b()
    cg[2].ys(-1)
    hg.sz()
    cg[3].zfm()
    cg[3].ys(1)
    cg[2].yfm(1)
    gho(0)
    ghw(0)
    cg[2].yfm(-1)
    xs[0].x1a()
    xs[1].x2p()
    xs[1].x2m()
    xs[0].x1c()
    cg[2].yfp(2)
    hg.l0()
    cg[3].yfm(-1)
    xs[0].x1b()
    cg[3].yfm(1)
    xs[0].x2m()
    xs[0].x2p()
    cg[2].fin()
    gho(2)
    cgi.zfm()
    cgi.sy()
    xs[1].x3()
    cg[3].zl()
    ghw(2)
    xs[2].x1a()
    xs[2].x1b()
    xs[2].x1c()
    xs[0].x3()
    xs[1].grads()
    rg[1].sx()
    xs[2].x2p()
    rg[1].sz()
    cg[3].yfp(2)
    rg[1].sc()
    xs[0].grads()
    cgi.zfp()
    cgi.ys(-1)
    rg[0].sx()
    cg[3].fin()
    rg[1].f0p()
    rg[1].f0m()
    cgi.ys(1)
    gho(3)
    cgi.yfp(0)
    rg[0].sc()
    rg[1].s10()
    ghw(3)
    xs[3].x1a()
    xs[2].x2m()
    xs[3].x1c()
    xs[3].x1b()
    rg[0].sz()
    rg[0].f0p()
    rg[1].zx()
    cgi.yfm(-1)
    cgi.yfm(1)
    rg[1].l0()
    cgi.zl()
    rg[1].z2()
    xs[3].x2m()
    xs[2].x3()
    rg[0].l0()
    rg[0].z2()
    xs[3].x2p()
    xs[2].grads()
    cgi.yfp(2)
    rg[1].zc()
    rg[2].sx()
    rg[1].f1m()
    rg[0].zx()
    xs[3].x3()
    rg[0].f0m()
    rg[1].f1p()
    rg[2].sz()
    rg[1].l1()
    rg[1].fin()
    rg[2].sc()
    gi(1)
    ys[1].y1()
    rg[0].zc()
    xs[3].grads()
    ys[1].y1b()
    rg[2].f0p()
    rg[3].sx()
    rg[3].sz()
    rg[2].f0m()
    rg[0].f1m()
    rg[2].zx()
    rg[0].f1p()
    rg[2].s10()
    cgi.fin()
    rg[0].s10()
    rg[0].l1()
    rg[0].fin()
    gi(0)
    rg[3].f0m()
    ys[0].y1()
    rg[3].zx()
    rg[2].zc()
    ys[1].y2p()
    rg[2].l0()
    rg[2].z2()
    transpose_inputs()
    rg[3].sc()
    rg[2].f1m()
    ys[1].y2m()
    ys[0].y1b()
    gu(0)
    rg[3].f0p()
    ys[0].y2p()
    hg.zx()
    rg[2].l1()
    rg[2].f1p()
    rg[3].l0()
    rg[3].z2()
    ys[0].y2m()
    rg[2].fin()
    rg[3].zc()
    gi(2)
    ys[2].y1()
    rg[3].s10()
    hg.zc()
    rg[3].f1p()
    ys[1].y3()
    ys[0].y3()
    rg[3].f1m()
    ys[2].y1b()
    rg[3].l1()
    ys[2].y2m()
    ys[2].y2p()
    rg[3].fin()
    gi(3)
    ys[3].y1()
    ys[3].y1b()
    ys[0].y4p()
    ys[0].y4m()
    hg.f1m()
    hg.f1p()
    gu(2)
    ys[2].y3()
    ys[1].y4m()
    ys[3].y2m()
    ys[3].y2p()
    gu(3)
    ys[0].y5()
    ys[1].y4p()
    ys[3].y3()
    gu(1)
    ys[1].y5()
    hg.l1()
    ys[2].y4m()
    ys[2].y4p()
    ys[3].y4p()
    ys[3].y4m()
    hg.fin()
    grad_down()
    ys[3].y5()
    ys[2].y5()
    for c in sends:
        c.wait_send()


def per_device(inputs, cotangent, gate_pre, up_pre, w_gate, w_up, w_down):
    t, d = inputs.shape
    ff = gate_pre.shape[1]
    br = t // NH
    tokens = 16 * t
    scale = 1.0 / math.sqrt(tokens)

    def vm(*shape, kind=BF16):
        return pltpu.VMEM(shape, kind)

    scratch = [
        vm(NH, 2, 8, br, d), vm(NH, 2, 8, br, d), vm(d, tokens), vm(NH, 2, 8, br, ff), vm(NH, 2, 8, br, 2 * ff),
        vm(ff, d), vm(d, 2 * ff), vm(NH, br, ff), vm(NH, br, ff),
        vm(NH, 8, br, ff), vm(NH, 8, br, ff), vm(NH, 8, br, ff, kind=F32),
        vm(NH, 2, br, ff), vm(NH, 2, br, ff), vm(NH, 2, 2, br, ff), vm(NH, 2, 2, br, ff),
        vm(NH, br, ff, kind=F32), vm(NH, br, ff), vm(NH, br, ff),
        vm(NH, 2, 8, br, d, kind=F32),
        vm(NH, 2, 2, br, d), vm(NH, 2, 2, br, d), vm(NH, 2, 2, 2, br, d), vm(NH, 2, 2, 2, br, d),
        vm(NH, 2, 2, br, d, kind=F32),
        vm(NH, 2, br // 2, d), vm(NH, 2, br // 2, d), vm(NH, 2, 2, br // 2, d), vm(NH, 2, 2, br // 2, d),
        pltpu.SemaphoreType.DMA((N_SEM,)), pltpu.SemaphoreType.DMA((N_SEM,)), pltpu.SemaphoreType.DMA((16,)),
    ]
    hbm = pl.BlockSpec(memory_space=pl.ANY)
    gi, gg, gup, gd = pl.pallas_call(
        functools.partial(kernel, scale),
        out_shape=(
            pltpu.VMEM((NH, br, d), BF16), pltpu.VMEM((d, ff), F32), pltpu.VMEM((d, ff), F32), pltpu.VMEM((ff, d), F32),
        ),
        in_specs=[hbm] * 7,
        out_specs=(pl.BlockSpec(memory_space=pltpu.VMEM),) * 4,
        scratch_shapes=scratch,
        compiler_params=pltpu.CompilerParams(
            collective_id=0, has_side_effects=True, vmem_limit_bytes=VMEM_LIMIT
        ),
    )(
        inputs.reshape(NH, br, d), cotangent.reshape(NH, br, d), gate_pre.reshape(NH, br, ff),
        up_pre.reshape(NH, br, ff), w_gate, w_up, w_down,
    )
    return gi.reshape(t, d), gg, gup, gd


def solution(mesh):
    split = Mesh(mesh.devices.reshape(2, 4, 2, 4, 4), ROW + COL)
    in_specs = (P(COL, ROW), P(COL, ROW), P(ROW, COL), P(ROW, COL), P(ROW, COL), P(ROW, COL), P(COL, ROW))
    out_specs = (P(COL, ROW), P(ROW, COL), P(ROW, COL), P(COL, ROW))
    return jax.shard_map(per_device, mesh=split, in_specs=in_specs, out_specs=out_specs, check_vma=False)
```

```python
import functools
import math

import jax
import jax.numpy as jnp
from jax import lax
from jax.experimental import pallas as pl
from jax.experimental.pallas import tpu as pltpu
from jax.sharding import Mesh
from jax.sharding import PartitionSpec as P

ROW = ("zl", "x", "core")
COL = ("y", "zh")
SIZES = {"zl": 2, "x": 4, "core": 2, "y": 4, "zh": 4}
MESH = pl.DeviceIdType.MESH
F32, BF16 = jnp.float32, jnp.bfloat16
NH = 4
RG_MODE = ('A', 'A', 'A', 'A')
HG_MODE = '0'
N_SEM = 320
VMEM_LIMIT = 50 * 1024 * 1024
TN = 512


def nt(left, right):
    return lax.dot_general(left, right, (((1,), (1,)), ((), ())), preferred_element_type=F32)


def kernel(
    scale,
    inp_hbm, cot_hbm, gate_hbm, up_hbm, wg_hbm, wu_hbm, wd_hbm,
    OGI, OGG, OGU, OD,
    CT, IN, INT, HID, GU, WD, WGU, GATE, UP,
    PC, RC, S, XA, XAR, XB, XBR, R, ZS, ZR,
    GIP, YA, YAR, YB, YBR, R2, HB, HBR,
    ssem, rsem, lsem,
):
    at = {a: lax.axis_index(a) for a in SIZES}
    x, y, zh, zl, k = at["x"], at["y"], at["zh"], at["zl"], at["core"]
    br = CT.shape[3]

    def step(axis, d):
        return lax.rem(at[axis] + (d + SIZES[axis]), SIZES[axis])

    def peer(axis, d):
        return {axis: step(axis, d)}

    sends = []

    def send(src, dst, to):
        i = len(sends)
        c = pltpu.make_async_remote_copy(
            src_ref=src, dst_ref=dst, send_sem=ssem.at[i], recv_sem=rsem.at[i],
            device_id=to, device_id_type=MESH,
        )
        c.start()
        sends.append(c)
        return c

    n_local = [0]

    def local(src, dst):
        c = pltpu.make_async_copy(src, dst, lsem.at[n_local[0]])
        n_local[0] += 1
        c.start()
        return c

    ck, cb = lax.rem(zh, 2), 2 * y + zh // 2

    own_cot = local(cot_hbm, CT.at[:, ck, cb])
    load_gate = local(gate_hbm, GATE)
    load_up = local(up_hbm, UP)
    load_wd = local(wd_hbm, WD)
    own_inp = local(inp_hbm, IN.at[:, ck, cb])
    load_wg = local(wg_hbm, WGU.at[:, pl.ds(0, 1024)])
    load_wu = local(wu_hbm, WGU.at[:, pl.ds(1024, 1024)])

    barrier = pltpu.get_barrier_semaphore()
    peers = [peer("x", 1), peer("x", -1), peer("y", 1), peer("y", -1), peer("zh", 1), peer("zh", -1),
             peer("zh", 2), peer("zl", 1), peer("core", 1)]
    for p in peers:
        pl.semaphore_signal(barrier, inc=1, device_id=p, device_id_type=MESH)
    pl.semaphore_wait(barrier, len(peers))

    class ColGather:
        def __init__(self, block, halves):
            self.block, self.halves = block, halves
            self.y, self.f = {}, {}

        def at(self, dy, dz):
            yy, zz = step("y", dy), step("zh", dz)
            return self.block(lax.rem(zz, 2), 2 * yy + zz // 2)

        def ysend(self, dz):
            b = self.at(0, dz)
            self.y[dz] = (send(b, b, peer("y", 1)), send(b, b, peer("y", -1)))

        def sz(self):
            b = self.at(0, 0)
            self.z1 = (send(b, b, peer("zh", 1)), send(b, b, peer("zh", -1)))

        def sy(self):
            self.ysend(0)

        def zfp(self):
            self.z1[0].wait_recv()
            b = self.halves(self.at(0, -1))[0]
            self.z2p = send(b, b, peer("zh", 1))

        def zfm(self):
            self.z1[1].wait_recv()
            b = self.halves(self.at(0, 1))[1]
            self.z2m = send(b, b, peer("zh", -1))

        def ys(self, dz):
            self.ysend(dz)

        def zl(self):
            self.z2p.wait_recv()
            self.z2m.wait_recv()
            self.ysend(2)

        def yfp(self, dz):
            self.y[dz][0].wait_recv()
            b = self.at(-1, dz)
            self.f[dz] = send(b, b, peer("y", 1))

        def yfm(self, dz):
            self.y[dz][1].wait_recv()
            b = self.at(1, dz)
            self.f[dz] = send(b, b, peer("y", -1))

        def fin(self):
            for dz in (0, 2):
                self.y[dz][1].wait_recv()
            for dz in (1, -1):
                self.y[dz][0].wait_recv()
            for c in self.f.values():
                c.wait_recv()

    def row_halves(ref):
        return ref.at[pl.ds(0, br // 2)], ref.at[pl.ds(br // 2, br // 2)]

    def piece_halves(ref):
        return ref.at[pl.ds(0, NH // 2)], ref.at[pl.ds(NH // 2, NH // 2)]

    cg = [ColGather(lambda q, b, h=h: CT.at[h, q, b], row_halves) for h in range(NH)]
    cgi = ColGather(lambda q, b: IN.at[:, q, b], piece_halves)

    class RowGather:
        def __init__(self, block, mode, mirror):
            self.block, self.mode, self.mirror = block, mode, mirror
            self.core = []

        def at(self, dx, dzl):
            return self.block(k, step("zl", dzl) * 4 + step("x", dx))

        def to(self, dx, dzl, axis, d=1):
            b = self.at(dx, dzl)
            return send(b, b, peer(axis, d))

        def share(self, dx, dzl):
            self.core.append(self.to(dx, dzl, "core"))

        def sz(self):
            self.z = self.to(0, 0, "zl")

        def sx(self):
            self.x0 = (self.to(0, 0, "x", 1), self.to(0, 0, "x", -1))

        def sc(self):
            self.share(0, 0)

        def f0p(self):
            self.x0[0].wait_recv()
            if not self.mirror:
                self.f0 = self.to(-1, 0, "x", 1)

        def s10(self):
            self.share(-1, 0)

        def f0m(self):
            self.x0[1].wait_recv()
            if self.mirror:
                self.f0 = self.to(1, 0, "x", -1)
            self.share(1, 0)

        def l0(self):
            self.f0.wait_recv()
            self.share(2, 0)

        def zx(self):
            self.z.wait_recv()
            up = self.to(0, 1, "x", 1) if self.mode != "B" else None
            self.x1 = (up, self.to(0, 1, "x", -1))

        def zc(self):
            self.share(0, 1)

        def zp(self):
            self.z1 = self.to(-1, 0, "zl")

        def z2(self):
            self.f1 = self.to(2, 0, "zl")

        def f1p(self):
            (self.z1 if self.mode == "B" else self.x1[0]).wait_recv()
            self.share(-1, 1)

        def f1m(self):
            self.x1[1].wait_recv()
            if self.mode == "0":
                self.f1 = self.to(1, 1, "x", -1)
            self.share(1, 1)

        def l1(self):
            self.f1.wait_recv()
            self.share(2, 1)

        def fin(self):
            for c in self.core:
                c.wait_recv()

    hg = RowGather(lambda q, b: HID.at[:, q, b], HG_MODE, False)
    rg = [RowGather(lambda q, b, h=h: GU.at[h, q, b], RG_MODE[h], RG_MODE[h] == "A" and h % 2 == 1) for h in range(NH)]

    ready = []

    def when(*copies):
        for c in copies:
            if id(c) not in ready:
                ready.append(id(c))
                c.wait()

    def hidden():
        when(load_gate, load_up)

        @pl.loop(0, NH * br // 32)
        def _(i):
            h, s = i // (br // 32), pl.multiple_of(lax.rem(i, br // 32) * 32, 32)
            g = GATE[h, pl.ds(s, 32)].astype(F32)
            u = UP[h, pl.ds(s, 32)].astype(F32)
            HID[h, k, zl * 4 + x, pl.ds(s, 32)] = (g * jax.nn.sigmoid(g) * u).astype(BF16)

    core_part = {}

    def gho(h):
        when(load_wd)

        @pl.loop(0, 1024 // TN)
        def _(n):
            c = pl.multiple_of(n * TN, TN)
            a = CT[h, 1 - k].reshape(8 * br, CT.shape[4])
            p = nt(a, WD[pl.ds(c, TN), :])
            PC[h, :, :, pl.ds(c, TN)] = p.astype(PC.dtype).reshape(8, br, TN)

        core_part[h] = send(PC.at[h], RC.at[h], peer("core", 1))

    def ghw(h):
        @pl.loop(0, 1024 // TN)
        def _(n):
            c = pl.multiple_of(n * TN, TN)
            a = CT[h, k].reshape(8 * br, CT.shape[4])
            S[h, :, :, pl.ds(c, TN)] = nt(a, WD[pl.ds(c, TN), :]).reshape(8, br, TN)

    class XScatter:
        def __init__(self, h):
            self.h = h

        def part(self, dx, z):
            return z * 4 + step("x", dx)

        def total(self, b):
            return S[self.h, b] + RC[self.h, b].astype(F32)

        def x1a(self):
            h = self.h
            core_part[h].wait_recv()
            for z in range(2):
                XA[h, z] = self.total(self.part(2, z)).astype(BF16)
            self.a = (send(XA.at[h, 0], XAR.at[h, 0], peer("x", 1)), send(XA.at[h, 1], XAR.at[h, 1], peer("x", -1)))

        def x1c(self):
            h = self.h
            XB[h, 0, 1] = self.total(self.part(1, 1)).astype(BF16)
            XB[h, 1, 0] = self.total(self.part(-1, 0)).astype(BF16)
            self.b1 = (send(XB.at[h, 0, 1], XBR.at[h, 0, 1], peer("x", 1)),
                       send(XB.at[h, 1, 0], XBR.at[h, 1, 0], peer("x", -1)))

        def x1b(self):
            for b in (self.part(1, 0), self.part(-1, 1), self.part(0, 0), self.part(0, 1)):
                S[self.h, b] = self.total(b)

        def x2p(self):
            h = self.h
            self.a[0].wait_recv()
            XB[h, 0, 0] = (S[h, self.part(1, 0)] + XAR[h, 0].astype(F32)).astype(BF16)
            self.b2p = send(XB.at[h, 0, 0], XBR.at[h, 0, 0], peer("x", 1))

        def x2m(self):
            h = self.h
            self.a[1].wait_recv()
            XB[h, 1, 1] = (S[h, self.part(-1, 1)] + XAR[h, 1].astype(F32)).astype(BF16)
            self.b2m = send(XB.at[h, 1, 1], XBR.at[h, 1, 1], peer("x", -1))

        def x3(self):
            h = self.h
            for c in self.b1 + (self.b2p, self.b2m):
                c.wait_recv()

            def total(z):
                return S[h, self.part(0, z)] + XBR[h, 0, z].astype(F32) + XBR[h, 1, z].astype(F32)

            ZS[h] = total(1 - zl).astype(ZS.dtype)
            self.z = send(ZS.at[h], ZR.at[h], peer("zl", 1))
            R[h] = total(zl)

        def grads(self):
            h = self.h
            self.z.wait_recv()

            @pl.loop(0, br // 16)
            def _(i):
                s = pl.multiple_of(i * 16, 16)
                gh = R[h, pl.ds(s, 16)] + ZR[h, pl.ds(s, 16)].astype(F32)
                g = GATE[h, pl.ds(s, 16)].astype(F32)
                u = UP[h, pl.ds(s, 16)].astype(F32)
                sig = jax.nn.sigmoid(g)
                b = zl * 4 + x
                GU[h, k, b, pl.ds(s, 16), pl.ds(0, 1024)] = (gh * u * sig * (1.0 + g * (1.0 - sig))).astype(BF16)
                GU[h, k, b, pl.ds(s, 16), pl.ds(1024, 1024)] = (gh * (g * sig)).astype(BF16)

    xs = [XScatter(h) for h in range(NH)]

    def gi(h):
        when(load_wg, load_wu)

        @pl.loop(0, 2)
        def _(q):
            @pl.loop(0, 512 // TN)
            def _(i):
                c = pl.multiple_of(i * TN, TN)
                a = GU[h, q].reshape(8 * br, GU.shape[4])
                GIP[h, q, :, :, pl.ds(c, TN)] = nt(a, WGU[pl.ds(c, TN), :]).reshape(8, br, TN)

    class YScatter:
        def __init__(self, h):
            self.h = h

        def part(self, dy, q):
            return GIP[self.h, q, pl.ds(2 * step("y", dy), 2)]

        def y1(self):
            h = self.h
            for q in range(2):
                YA[h, q] = self.part(2, q).astype(BF16)
            self.a = (send(YA.at[h, 0], YAR.at[h, 0], peer("y", 1)), send(YA.at[h, 1], YAR.at[h, 1], peer("y", -1)))

        def y1b(self):
            h = self.h
            YB[h, 0, 1] = self.part(1, 1).astype(BF16)
            YB[h, 1, 0] = self.part(-1, 0).astype(BF16)
            self.b1 = (send(YB.at[h, 0, 1], YBR.at[h, 0, 1], peer("y", 1)),
                       send(YB.at[h, 1, 0], YBR.at[h, 1, 0], peer("y", -1)))

        def y2p(self):
            h = self.h
            self.a[0].wait_recv()
            YB[h, 0, 0] = (self.part(1, 0) + YAR[h, 0].astype(F32)).astype(BF16)
            self.b2p = send(YB.at[h, 0, 0], YBR.at[h, 0, 0], peer("y", 1))

        def y2m(self):
            h = self.h
            self.a[1].wait_recv()
            YB[h, 1, 1] = (self.part(-1, 1) + YAR[h, 1].astype(F32)).astype(BF16)
            self.b2m = send(YB.at[h, 1, 1], YBR.at[h, 1, 1], peer("y", -1))

        def y3(self):
            h = self.h
            for c in self.b1 + (self.b2p, self.b2m):
                c.wait_recv()
            for q in range(2):
                R2[h, q] = self.part(0, q) + YBR[h, 0, q].astype(F32) + YBR[h, 1, q].astype(F32)

            def zpart(dz):
                zz = step("zh", dz)
                return R2[h, lax.rem(zz, 2), zz // 2]

            self.zpart = zpart
            self.zs = []
            for i, dz in enumerate((2, 1, -1)):
                HB[h, i] = zpart(dz).astype(BF16)
                self.zs.append(send(HB.at[h, i], HBR.at[h, i], peer("zh", dz)))

        def y5(self):
            h = self.h
            for c in self.zs:
                c.wait_recv()
            OGI[h] = (
                (self.zpart(0) + HBR[h, 1].astype(F32)) + (HBR[h, 2].astype(F32) + HBR[h, 0].astype(F32))
            ).astype(BF16)

    ys = [YScatter(h) for h in range(NH)]

    def transpose_inputs():
        @pl.loop(0, NH * 2)
        def _(i):
            rows = 8 * br
            v = IN[i // 2, lax.rem(i, 2)].reshape(rows, IN.shape[4])
            INT[:, pl.ds(pl.multiple_of(i * rows, rows), rows)] = v.T

    def grad_down():
        @pl.loop(0, 4)
        def _(i):
            c = pl.multiple_of(i * 256, 256)
            a = HID[:, :, :, :, pl.ds(c, 256)].reshape(NH * 16 * br, 256)
            b = CT[...].reshape(NH * 16 * br, CT.shape[4])
            p = lax.dot_general(a, b, (((0,), (0,)), ((), ())), preferred_element_type=F32)
            OD[pl.ds(c, 256), :] = p * scale

    added = []

    def gu(h):
        rows = 16 * br
        first, last = not added, len(added) == NH - 1
        added.append(h)

        for out, base in ((OGG, 0), (OGU, 1024)):
            @pl.loop(0, 4)
            def _(i):
                c = pl.multiple_of(i * 256, 256)
                from_gu = pl.ds(pl.multiple_of(base + i * 256, 256), 256)
                p = jnp.dot(INT[:, pl.ds(h * rows, rows)], GU[h, :, :, :, from_gu].reshape(rows, 256),
                            preferred_element_type=F32)
                if not first:
                    p = p + out[:, pl.ds(c, 256)]
                out[:, pl.ds(c, 256)] = p * scale if last else p

    own_cot.wait()
    own_inp.wait()
    cg[0].sz()
    hidden()
    cg[2].sy()
    hg.sx()
    cg[2].sz()
    cg[0].sy()
    cg[3].sy()
    cg[3].sz()
    cg[0].zfp()
    cg[0].zfm()
    cg[0].ys(1)
    cg[0].ys(-1)
    cg[2].zfp()
    cg[2].zfm()
    cg[1].sz()
    cg[2].ys(1)
    cg[2].ys(-1)
    cg[3].zfp()
    cg[3].ys(-1)
    cg[0].yfm(1)
    cg[0].zl()
    cg[3].zfm()
    cg[0].yfp(0)
    hg.f0p()
    cg[2].zl()
    cg[2].yfm(1)
    cg[2].yfp(0)
    cg[0].yfm(-1)
    cg[0].yfp(2)
    cg[1].zfp()
    cg[1].zfm()
    hg.f0m()
    cg[3].zl()
    cg[2].yfp(2)
    cgi.sz()
    cg[2].yfm(-1)
    cg[3].ys(1)
    cg[3].yfp(0)
    cg[1].ys(1)
    cg[1].sy()
    cg[0].fin()
    gho(0)
    cg[1].ys(-1)
    ghw(0)
    cg[3].yfm(-1)
    cg[3].yfp(2)
    cg[2].fin()
    gho(2)
    cg[3].yfm(1)
    cg[1].zl()
    xs[0].x1a()
    xs[0].x1c()
    hg.sz()
    ghw(2)
    xs[2].x1a()
    xs[2].x1c()
    hg.l0()
    cg[1].yfm(-1)
    xs[0].x1b()
    cg[1].yfm(1)
    cg[1].yfp(0)
    cg[1].yfp(2)
    cg[3].fin()
    gho(3)
    xs[0].x2m()
    xs[0].x2p()
    xs[2].x1b()
    ghw(3)
    xs[3].x1a()
    xs[3].x1b()
    xs[3].x1c()
    cgi.zfp()
    cgi.zfm()
    cgi.ys(1)
    xs[2].x2p()
    cg[1].fin()
    gho(1)
    ghw(1)
    xs[2].x2m()
    xs[0].x3()
    xs[1].x1a()
    xs[3].x2m()
    cgi.ys(-1)
    xs[1].x1b()
    xs[1].x1c()
    xs[3].x2p()
    xs[2].x3()
    xs[0].grads()
    rg[0].sx()
    cgi.sy()
    xs[1].x2p()
    rg[0].sz()
    xs[1].x2m()
    xs[3].x3()
    cgi.zl()
    xs[2].grads()
    rg[2].sx()
    rg[2].sz()
    rg[0].f0p()
    hg.sc()
    rg[0].zx()
    cgi.yfm(-1)
    xs[1].x3()
    xs[3].grads()
    rg[2].sc()
    rg[3].sz()
    rg[0].f0m()
    cgi.yfp(0)
    rg[2].f0p()
    rg[3].sx()
    xs[1].grads()
    rg[2].zx()
    rg[1].sx()
    cgi.yfp(2)
    rg[2].f0m()
    rg[0].s10()
    rg[0].l0()
    rg[0].z2()
    rg[1].sz()
    cgi.yfm(1)
    rg[2].l0()
    rg[2].z2()
    rg[3].f0m()
    rg[2].s10()
    rg[0].f1m()
    rg[0].zc()
    cgi.fin()
    rg[0].f1p()
    rg[3].sc()
    transpose_inputs()
    rg[1].sc()
    rg[0].l1()
    rg[0].sc()
    rg[3].f0p()
    rg[1].f0m()
    rg[2].zc()
    rg[3].zx()
    rg[0].fin()
    gi(0)
    ys[0].y1()
    rg[1].zx()
    rg[2].f1m()
    rg[2].f1p()
    rg[3].s10()
    ys[0].y1b()
    rg[2].l1()
    rg[3].l0()
    rg[3].z2()
    gu(0)
    rg[2].fin()
    gi(2)
    ys[2].y1()
    hg.zx()
    ys[0].y2m()
    rg[1].l0()
    rg[1].z2()
    hg.zc()
    ys[2].y1b()
    rg[1].zc()
    ys[0].y2p()
    rg[3].l1()
    rg[3].f1m()
    rg[3].zc()
    rg[1].f0p()
    rg[1].s10()
    rg[3].f1p()
    gu(2)
    rg[1].f1m()
    rg[1].f1p()
    rg[3].fin()
    ys[2].y2p()
    ys[2].y2m()
    gi(3)
    rg[1].l1()
    ys[3].y1()
    ys[3].y1b()
    ys[0].y3()
    rg[1].fin()
    gi(1)
    ys[1].y1()
    hg.f1m()
    ys[2].y3()
    ys[3].y2m()
    hg.f1p()
    ys[3].y2p()
    ys[1].y1b()
    gu(3)
    ys[1].y2m()
    ys[1].y2p()
    hg.s10()
    ys[3].y3()
    gu(1)
    ys[1].y3()
    hg.l1()
    ys[2].y5()
    hg.fin()
    grad_down()
    ys[0].y5()
    ys[3].y5()
    ys[1].y5()
    for c in sends:
        c.wait_send()


def put_out(a, b, c, d, ao, bo, co, do, sem):
    copies = [pltpu.make_async_copy(f, t, sem.at[i]) for i, (f, t) in enumerate(((d, do), (b, bo), (c, co), (a, ao)))]
    for c in copies:
        c.start()
    for c in copies:
        c.wait()


def per_device(inputs, cotangent, gate_pre, up_pre, w_gate, w_up, w_down):
    t, d = inputs.shape
    ff = gate_pre.shape[1]
    br = t // NH
    tokens = 16 * t
    scale = 1.0 / math.sqrt(tokens)

    def vm(*shape, kind=BF16):
        return pltpu.VMEM(shape, kind)

    scratch = [
        vm(NH, 2, 8, br, d), vm(NH, 2, 8, br, d), vm(d, tokens), vm(NH, 2, 8, br, ff), vm(NH, 2, 8, br, 2 * ff),
        vm(ff, d), vm(d, 2 * ff), vm(NH, br, ff), vm(NH, br, ff),
        vm(NH, 8, br, ff), vm(NH, 8, br, ff), vm(NH, 8, br, ff, kind=F32),
        vm(NH, 2, br, ff), vm(NH, 2, br, ff), vm(NH, 2, 2, br, ff), vm(NH, 2, 2, br, ff),
        vm(NH, br, ff, kind=F32), vm(NH, br, ff), vm(NH, br, ff),
        vm(NH, 2, 8, br, d, kind=F32),
        vm(NH, 2, 2, br, d), vm(NH, 2, 2, br, d), vm(NH, 2, 2, 2, br, d), vm(NH, 2, 2, 2, br, d),
        vm(NH, 2, 2, br, d, kind=F32),
        vm(NH, 3, br, d), vm(NH, 3, br, d),
        pltpu.SemaphoreType.DMA((N_SEM,)), pltpu.SemaphoreType.DMA((N_SEM,)), pltpu.SemaphoreType.DMA((16,)),
    ]
    hbm = pl.BlockSpec(memory_space=pl.ANY)
    gi, gg, gup, gd = pl.pallas_call(
        functools.partial(kernel, scale),
        out_shape=(
            pltpu.VMEM((NH, br, d), BF16), pltpu.VMEM((d, ff), F32), pltpu.VMEM((d, ff), F32), pltpu.VMEM((ff, d), F32),
        ),
        in_specs=[hbm] * 7,
        out_specs=(pl.BlockSpec(memory_space=pltpu.VMEM),) * 4,
        scratch_shapes=scratch,
        compiler_params=pltpu.CompilerParams(
            collective_id=0, has_side_effects=True, vmem_limit_bytes=VMEM_LIMIT
        ),
    )(
        inputs.reshape(NH, br, d), cotangent.reshape(NH, br, d), gate_pre.reshape(NH, br, ff),
        up_pre.reshape(NH, br, ff), w_gate, w_up, w_down,
    )
    vmem = pl.BlockSpec(memory_space=pltpu.VMEM)
    gi, gg, gup, gd = pl.pallas_call(
        put_out,
        out_shape=(
            jax.ShapeDtypeStruct((NH, br, d), BF16),
            jax.ShapeDtypeStruct((d, ff), F32),
            jax.ShapeDtypeStruct((d, ff), F32),
            jax.ShapeDtypeStruct((ff, d), F32),
        ),
        in_specs=[vmem] * 4,
        out_specs=(hbm,) * 4,
        scratch_shapes=[pltpu.SemaphoreType.DMA((4,))],
        compiler_params=pltpu.CompilerParams(vmem_limit_bytes=1024 * 1024),
    )(gi, gg, gup, gd)
    return gi.reshape(t, d), gg, gup, gd


def solution(mesh):
    split = Mesh(mesh.devices.reshape(2, 4, 2, 4, 4), ROW + COL)
    in_specs = (P(COL, ROW), P(COL, ROW), P(ROW, COL), P(ROW, COL), P(ROW, COL), P(ROW, COL), P(COL, ROW))
    out_specs = (P(COL, ROW), P(ROW, COL), P(ROW, COL), P(COL, ROW))
    return jax.shard_map(per_device, mesh=split, in_specs=in_specs, out_specs=out_specs, check_vma=False)
```

```python
import functools
import math

import jax
import jax.numpy as jnp
from jax import lax
from jax.experimental import pallas as pl
from jax.experimental.pallas import tpu as pltpu
from jax.sharding import Mesh
from jax.sharding import PartitionSpec as P

ROW = ("zl", "x", "core")
COL = ("y", "zh")
SIZES = {"zl": 2, "x": 4, "core": 2, "y": 4, "zh": 4}
MESH = pl.DeviceIdType.MESH
F32, BF16 = jnp.float32, jnp.bfloat16
NH = 4
RG_MODE = ('A', 'A', 'A', 'A')
HG_MODE = '0'
CG_DIRECT = (0,)
Y_DIRECT = (3,)
N_SEM = 320
VMEM_LIMIT = 50 * 1024 * 1024
TN = 512


def nt(left, right):
    return lax.dot_general(left, right, (((1,), (1,)), ((), ())), preferred_element_type=F32)


def kernel(
    scale,
    inp_hbm, cot_hbm, gate_hbm, up_hbm, wg_hbm, wu_hbm, wd_hbm,
    OGI, OGG, OGU, OD,
    CT, IN, INT, HID, GU, WD, WGU, GATE, UP,
    PC, RC, S, XA, XAR, XB, XBR, R, ZS, ZR,
    GIP, YA, YAR, YB, YBR, R2, HB, HBR, YD, YDR,
    ssem, rsem, lsem,
):
    at = {a: lax.axis_index(a) for a in SIZES}
    x, y, zh, zl, k = at["x"], at["y"], at["zh"], at["zl"], at["core"]
    br = CT.shape[3]

    def step(axis, d):
        return lax.rem(at[axis] + (d + SIZES[axis]), SIZES[axis])

    def peer(axis, d):
        return {axis: step(axis, d)}

    sends = []

    def send(src, dst, to):
        i = len(sends)
        c = pltpu.make_async_remote_copy(
            src_ref=src, dst_ref=dst, send_sem=ssem.at[i], recv_sem=rsem.at[i],
            device_id=to, device_id_type=MESH,
        )
        c.start()
        sends.append(c)
        return c

    n_local = [0]

    def local(src, dst):
        c = pltpu.make_async_copy(src, dst, lsem.at[n_local[0]])
        n_local[0] += 1
        c.start()
        return c

    ck, cb = lax.rem(zh, 2), 2 * y + zh // 2

    own_cot = local(cot_hbm, CT.at[:, ck, cb])
    load_gate = local(gate_hbm, GATE)
    load_up = local(up_hbm, UP)
    load_wd = local(wd_hbm, WD)
    own_inp = local(inp_hbm, IN.at[:, ck, cb])
    load_wg = local(wg_hbm, WGU.at[:, pl.ds(0, 1024)])
    load_wu = local(wu_hbm, WGU.at[:, pl.ds(1024, 1024)])

    barrier = pltpu.get_barrier_semaphore()
    peers = [peer("x", 1), peer("x", -1), peer("y", 1), peer("y", -1), peer("zh", 1), peer("zh", -1),
             peer("y", 2), peer("zh", 2), peer("zl", 1), peer("core", 1)]
    for p in peers:
        pl.semaphore_signal(barrier, inc=1, device_id=p, device_id_type=MESH)
    pl.semaphore_wait(barrier, len(peers))

    class ColGather:
        def __init__(self, block, halves, direct=False):
            self.block, self.halves, self.direct = block, halves, direct
            self.y, self.f = {}, {}

        def at(self, dy, dz):
            yy, zz = step("y", dy), step("zh", dz)
            return self.block(lax.rem(zz, 2), 2 * yy + zz // 2)

        def ysend(self, dz):
            b = self.at(0, dz)
            self.y[dz] = (send(b, b, peer("y", 1)), send(b, b, peer("y", -1)))
            if self.direct:
                self.f[dz] = send(b, b, peer("y", 2))

        def sz(self):
            b = self.at(0, 0)
            self.z1 = (send(b, b, peer("zh", 1)), send(b, b, peer("zh", -1)))
            if self.direct:
                self.z2p = send(b, b, peer("zh", 2))

        def sy(self):
            self.ysend(0)

        def zfp(self):
            self.z1[0].wait_recv()
            if self.direct:
                return
            b = self.halves(self.at(0, -1))[0]
            self.z2p = send(b, b, peer("zh", 1))

        def zfm(self):
            self.z1[1].wait_recv()
            if self.direct:
                return
            b = self.halves(self.at(0, 1))[1]
            self.z2m = send(b, b, peer("zh", -1))

        def ys(self, dz):
            self.ysend(dz)

        def zl(self):
            self.z2p.wait_recv()
            if not self.direct:
                self.z2m.wait_recv()
            self.ysend(2)

        def yfp(self, dz):
            self.y[dz][0].wait_recv()
            b = self.at(-1, dz)
            self.f[dz] = send(b, b, peer("y", 1))

        def yfm(self, dz):
            self.y[dz][1].wait_recv()
            b = self.at(1, dz)
            self.f[dz] = send(b, b, peer("y", -1))

        def fin(self):
            for dz in self.y:
                if self.direct or dz in (0, 2):
                    self.y[dz][1].wait_recv()
                if self.direct or dz in (1, -1):
                    self.y[dz][0].wait_recv()
            for c in self.f.values():
                c.wait_recv()

    def row_halves(ref):
        return ref.at[pl.ds(0, br // 2)], ref.at[pl.ds(br // 2, br // 2)]

    def piece_halves(ref):
        return ref.at[pl.ds(0, NH // 2)], ref.at[pl.ds(NH // 2, NH // 2)]

    cg = [ColGather(lambda q, b, h=h: CT.at[h, q, b], row_halves, h in CG_DIRECT) for h in range(NH)]
    cgi = ColGather(lambda q, b: IN.at[:, q, b], piece_halves)

    class RowGather:
        def __init__(self, block, mode, mirror):
            self.block, self.mode, self.mirror = block, mode, mirror
            self.core = []

        def at(self, dx, dzl):
            return self.block(k, step("zl", dzl) * 4 + step("x", dx))

        def to(self, dx, dzl, axis, d=1):
            b = self.at(dx, dzl)
            return send(b, b, peer(axis, d))

        def share(self, dx, dzl):
            self.core.append(self.to(dx, dzl, "core"))

        def sz(self):
            self.z = self.to(0, 0, "zl")

        def sx(self):
            self.x0 = (self.to(0, 0, "x", 1), self.to(0, 0, "x", -1))

        def sc(self):
            self.share(0, 0)

        def f0p(self):
            self.x0[0].wait_recv()
            if not self.mirror:
                self.f0 = self.to(-1, 0, "x", 1)

        def s10(self):
            self.share(-1, 0)

        def f0m(self):
            self.x0[1].wait_recv()
            if self.mirror:
                self.f0 = self.to(1, 0, "x", -1)
            self.share(1, 0)

        def l0(self):
            self.f0.wait_recv()
            self.share(2, 0)

        def zx(self):
            self.z.wait_recv()
            up = self.to(0, 1, "x", 1) if self.mode != "B" else None
            self.x1 = (up, self.to(0, 1, "x", -1))

        def zc(self):
            self.share(0, 1)

        def zp(self):
            self.z1 = self.to(-1, 0, "zl")

        def z2(self):
            self.f1 = self.to(2, 0, "zl")

        def f1p(self):
            (self.z1 if self.mode == "B" else self.x1[0]).wait_recv()
            self.share(-1, 1)

        def f1m(self):
            self.x1[1].wait_recv()
            if self.mode == "0":
                self.f1 = self.to(1, 1, "x", -1)
            self.share(1, 1)

        def l1(self):
            self.f1.wait_recv()
            self.share(2, 1)

        def fin(self):
            for c in self.core:
                c.wait_recv()

    hg = RowGather(lambda q, b: HID.at[:, q, b], HG_MODE, False)
    rg = [RowGather(lambda q, b, h=h: GU.at[h, q, b], RG_MODE[h], RG_MODE[h] == "A" and h % 2 == 1) for h in range(NH)]

    ready = []

    def when(*copies):
        for c in copies:
            if id(c) not in ready:
                ready.append(id(c))
                c.wait()

    def hidden():
        when(load_gate, load_up)

        @pl.loop(0, NH * br // 32)
        def _(i):
            h, s = i // (br // 32), pl.multiple_of(lax.rem(i, br // 32) * 32, 32)
            g = GATE[h, pl.ds(s, 32)].astype(F32)
            u = UP[h, pl.ds(s, 32)].astype(F32)
            HID[h, k, zl * 4 + x, pl.ds(s, 32)] = (g * jax.nn.sigmoid(g) * u).astype(BF16)

    core_part = {}

    def gho(h):
        when(load_wd)

        @pl.loop(0, 1024 // TN)
        def _(n):
            c = pl.multiple_of(n * TN, TN)
            a = CT[h, 1 - k].reshape(8 * br, CT.shape[4])
            p = nt(a, WD[pl.ds(c, TN), :])
            PC[h, :, :, pl.ds(c, TN)] = p.astype(PC.dtype).reshape(8, br, TN)

        core_part[h] = send(PC.at[h], RC.at[h], peer("core", 1))

    def ghw(h):
        @pl.loop(0, 1024 // TN)
        def _(n):
            c = pl.multiple_of(n * TN, TN)
            a = CT[h, k].reshape(8 * br, CT.shape[4])
            S[h, :, :, pl.ds(c, TN)] = nt(a, WD[pl.ds(c, TN), :]).reshape(8, br, TN)

    class XScatter:
        def __init__(self, h):
            self.h = h

        def part(self, dx, z):
            return z * 4 + step("x", dx)

        def total(self, b):
            return S[self.h, b] + RC[self.h, b].astype(F32)

        def x1a(self):
            h = self.h
            core_part[h].wait_recv()
            for z in range(2):
                XA[h, z] = self.total(self.part(2, z)).astype(BF16)
            self.a = (send(XA.at[h, 0], XAR.at[h, 0], peer("x", 1)), send(XA.at[h, 1], XAR.at[h, 1], peer("x", -1)))

        def x1c(self):
            h = self.h
            XB[h, 0, 1] = self.total(self.part(1, 1)).astype(BF16)
            XB[h, 1, 0] = self.total(self.part(-1, 0)).astype(BF16)
            self.b1 = (send(XB.at[h, 0, 1], XBR.at[h, 0, 1], peer("x", 1)),
                       send(XB.at[h, 1, 0], XBR.at[h, 1, 0], peer("x", -1)))

        def x1b(self):
            for b in (self.part(1, 0), self.part(-1, 1), self.part(0, 0), self.part(0, 1)):
                S[self.h, b] = self.total(b)

        def x2p(self):
            h = self.h
            self.a[0].wait_recv()
            XB[h, 0, 0] = (S[h, self.part(1, 0)] + XAR[h, 0].astype(F32)).astype(BF16)
            self.b2p = send(XB.at[h, 0, 0], XBR.at[h, 0, 0], peer("x", 1))

        def x2m(self):
            h = self.h
            self.a[1].wait_recv()
            XB[h, 1, 1] = (S[h, self.part(-1, 1)] + XAR[h, 1].astype(F32)).astype(BF16)
            self.b2m = send(XB.at[h, 1, 1], XBR.at[h, 1, 1], peer("x", -1))

        def x3(self):
            h = self.h
            for c in self.b1 + (self.b2p, self.b2m):
                c.wait_recv()

            def total(z):
                return S[h, self.part(0, z)] + XBR[h, 0, z].astype(F32) + XBR[h, 1, z].astype(F32)

            ZS[h] = total(1 - zl).astype(ZS.dtype)
            self.z = send(ZS.at[h], ZR.at[h], peer("zl", 1))
            R[h] = total(zl)

        def grads(self):
            h = self.h
            self.z.wait_recv()

            @pl.loop(0, br // 16)
            def _(i):
                s = pl.multiple_of(i * 16, 16)
                gh = R[h, pl.ds(s, 16)] + ZR[h, pl.ds(s, 16)].astype(F32)
                g = GATE[h, pl.ds(s, 16)].astype(F32)
                u = UP[h, pl.ds(s, 16)].astype(F32)
                sig = jax.nn.sigmoid(g)
                b = zl * 4 + x
                GU[h, k, b, pl.ds(s, 16), pl.ds(0, 1024)] = (gh * u * sig * (1.0 + g * (1.0 - sig))).astype(BF16)
                GU[h, k, b, pl.ds(s, 16), pl.ds(1024, 1024)] = (gh * (g * sig)).astype(BF16)

    xs = [XScatter(h) for h in range(NH)]

    def gi(h):
        when(load_wg, load_wu)

        @pl.loop(0, 2)
        def _(q):
            @pl.loop(0, 512 // TN)
            def _(i):
                c = pl.multiple_of(i * TN, TN)
                a = GU[h, q].reshape(8 * br, GU.shape[4])
                GIP[h, q, :, :, pl.ds(c, TN)] = nt(a, WGU[pl.ds(c, TN), :]).reshape(8, br, TN)

    class YScatter:
        def __init__(self, h):
            self.h = h

        def part(self, dy, q):
            return GIP[self.h, q, pl.ds(2 * step("y", dy), 2)]

        def y1(self):
            h = self.h
            if h in Y_DIRECT:
                self.d = []
                for i, dy in enumerate((2, 1, -1)):
                    for q in range(2):
                        YD[i, q] = self.part(dy, q).astype(BF16)
                    self.d.append(send(YD.at[i], YDR.at[i], peer("y", dy)))
                return
            for q in range(2):
                YA[h, q] = self.part(2, q).astype(BF16)
            self.a = (send(YA.at[h, 0], YAR.at[h, 0], peer("y", 1)), send(YA.at[h, 1], YAR.at[h, 1], peer("y", -1)))

        def y1b(self):
            h = self.h
            YB[h, 0, 1] = self.part(1, 1).astype(BF16)
            YB[h, 1, 0] = self.part(-1, 0).astype(BF16)
            self.b1 = (send(YB.at[h, 0, 1], YBR.at[h, 0, 1], peer("y", 1)),
                       send(YB.at[h, 1, 0], YBR.at[h, 1, 0], peer("y", -1)))

        def y2p(self):
            h = self.h
            self.a[0].wait_recv()
            YB[h, 0, 0] = (self.part(1, 0) + YAR[h, 0].astype(F32)).astype(BF16)
            self.b2p = send(YB.at[h, 0, 0], YBR.at[h, 0, 0], peer("y", 1))

        def y2m(self):
            h = self.h
            self.a[1].wait_recv()
            YB[h, 1, 1] = (self.part(-1, 1) + YAR[h, 1].astype(F32)).astype(BF16)
            self.b2m = send(YB.at[h, 1, 1], YBR.at[h, 1, 1], peer("y", -1))

        def y3(self):
            h = self.h
            if h in Y_DIRECT:
                for c in self.d:
                    c.wait_recv()
                for q in range(2):
                    R2[h, q] = (self.part(0, q) + YDR[1, q].astype(F32)) + (YDR[2, q].astype(F32) + YDR[0, q].astype(F32))
            else:
              for c in self.b1 + (self.b2p, self.b2m):
                c.wait_recv()
              for q in range(2):
                R2[h, q] = self.part(0, q) + YBR[h, 0, q].astype(F32) + YBR[h, 1, q].astype(F32)

            def zpart(dz):
                zz = step("zh", dz)
                return R2[h, lax.rem(zz, 2), zz // 2]

            self.zpart = zpart
            self.zs = []
            for i, dz in enumerate((2, 1, -1)):
                HB[h, i] = zpart(dz).astype(BF16)
                self.zs.append(send(HB.at[h, i], HBR.at[h, i], peer("zh", dz)))

        def y5(self):
            h = self.h
            for c in self.zs:
                c.wait_recv()
            OGI[h] = (
                (self.zpart(0) + HBR[h, 1].astype(F32)) + (HBR[h, 2].astype(F32) + HBR[h, 0].astype(F32))
            ).astype(BF16)

    ys = [YScatter(h) for h in range(NH)]

    def transpose_inputs():
        @pl.loop(0, NH * 2)
        def _(i):
            rows = 8 * br
            v = IN[i // 2, lax.rem(i, 2)].reshape(rows, IN.shape[4])
            INT[:, pl.ds(pl.multiple_of(i * rows, rows), rows)] = v.T

    def grad_down():
        @pl.loop(0, 4)
        def _(i):
            c = pl.multiple_of(i * 256, 256)
            a = HID[:, :, :, :, pl.ds(c, 256)].reshape(NH * 16 * br, 256)
            b = CT[...].reshape(NH * 16 * br, CT.shape[4])
            p = lax.dot_general(a, b, (((0,), (0,)), ((), ())), preferred_element_type=F32)
            OD[pl.ds(c, 256), :] = p * scale

    added = []

    def gu(h):
        rows = 16 * br
        first, last = not added, len(added) == NH - 1
        added.append(h)

        for out, base in ((OGG, 0), (OGU, 1024)):
            @pl.loop(0, 4)
            def _(i):
                c = pl.multiple_of(i * 256, 256)
                from_gu = pl.ds(pl.multiple_of(base + i * 256, 256), 256)
                p = jnp.dot(INT[:, pl.ds(h * rows, rows)], GU[h, :, :, :, from_gu].reshape(rows, 256),
                            preferred_element_type=F32)
                if not first:
                    p = p + out[:, pl.ds(c, 256)]
                out[:, pl.ds(c, 256)] = p * scale if last else p

    own_cot.wait()
    own_inp.wait()
    cg[1].sz()
    cg[0].sz()
    cg[1].sy()
    hidden()
    cg[2].sz()
    cg[2].sy()
    cg[3].sy()
    hg.sx()
    cg[0].sy()
    hg.sc()
    cg[1].yfp(0)
    cg[1].zfp()
    cg[1].ys(-1)
    cg[1].zfm()
    cg[1].ys(1)
    cg[3].sz()
    cg[0].zfp()
    cg[0].ys(-1)
    cg[0].zfm()
    cg[0].ys(1)
    cg[0].zl()
    cg[2].zfm()
    cg[2].zfp()
    cg[1].yfm(1)
    cg[1].zl()
    cg[2].yfp(0)
    hg.f0p()
    cg[2].ys(-1)
    cg[2].ys(1)
    cg[3].zfp()
    cg[3].zfm()
    cg[1].yfm(-1)
    cg[1].yfp(2)
    cgi.sz()
    cg[2].zl()
    cg[0].fin()
    gho(0)
    cg[3].ys(1)
    cg[3].ys(-1)
    hg.s10()
    cg[3].zl()
    hg.sz()
    cg[2].yfm(-1)
    ghw(0)
    xs[0].x1a()
    xs[0].x1c()
    cg[3].yfp(0)
    cg[2].yfm(1)
    cg[1].fin()
    gho(1)
    cg[2].yfp(2)
    cg[3].yfm(1)
    ghw(1)
    cg[3].yfm(-1)
    xs[1].x1a()
    xs[0].x1b()
    xs[1].x1c()
    xs[0].x2p()
    cg[3].yfp(2)
    xs[0].x2m()
    cg[2].fin()
    gho(2)
    ghw(2)
    cgi.zfm()
    cgi.ys(1)
    cgi.zfp()
    cgi.ys(-1)
    xs[2].x1a()
    hg.l0()
    cgi.sy()
    xs[1].x1b()
    xs[1].x2p()
    xs[1].x2m()
    cg[3].fin()
    xs[2].x1c()
    gho(3)
    xs[0].x3()
    xs[2].x1b()
    ghw(3)
    xs[3].x1a()
    xs[2].x2p()
    xs[2].x2m()
    xs[3].x1c()
    xs[1].x3()
    xs[0].grads()
    cgi.yfm(-1)
    rg[0].sx()
    rg[0].sc()
    rg[0].sz()
    xs[2].x3()
    xs[3].x1b()
    xs[3].x2p()
    xs[1].grads()
    rg[1].sz()
    rg[1].sx()
    cgi.zl()
    rg[1].sc()
    xs[3].x2m()
    rg[0].f0p()
    xs[2].grads()
    cgi.yfp(0)
    rg[2].sx()
    rg[2].sz()
    rg[1].f0m()
    rg[0].zx()
    rg[2].sc()
    xs[3].x3()
    rg[0].f0m()
    rg[1].zx()
    rg[1].zc()
    rg[0].l0()
    hg.f0m()
    rg[0].z2()
    xs[3].grads()
    rg[3].sc()
    rg[1].f0p()
    cgi.yfp(2)
    cgi.yfm(1)
    rg[2].f0p()
    rg[3].sx()
    rg[2].s10()
    rg[1].l0()
    rg[1].z2()
    rg[0].zc()
    rg[1].s10()
    rg[2].zx()
    rg[2].zc()
    rg[0].s10()
    rg[0].f1p()
    rg[3].sz()
    rg[0].f1m()
    rg[0].l1()
    rg[0].fin()
    gi(0)
    ys[0].y1()
    ys[0].y1b()
    rg[1].f1m()
    rg[2].f0m()
    rg[1].f1p()
    cgi.fin()
    transpose_inputs()
    rg[1].l1()
    rg[2].l0()
    rg[2].z2()
    rg[3].f0m()
    gu(0)
    rg[3].zx()
    ys[0].y2p()
    rg[2].f1m()
    rg[3].f0p()
    rg[1].fin()
    ys[0].y2m()
    gi(1)
    ys[1].y1()
    rg[2].l1()
    rg[2].f1p()
    rg[3].s10()
    rg[3].l0()
    rg[3].z2()
    ys[1].y1b()
    rg[3].zc()
    hg.zx()
    hg.zc()
    rg[2].fin()
    gi(2)
    ys[2].y1()
    rg[3].f1p()
    ys[2].y1b()
    rg[3].f1m()
    gu(2)
    rg[3].l1()
    ys[1].y2p()
    ys[1].y2m()
    ys[0].y3()
    ys[2].y2p()
    ys[2].y2m()
    rg[3].fin()
    gi(3)
    ys[3].y1()
    hg.f1m()
    hg.f1p()
    ys[1].y3()
    gu(3)
    ys[2].y3()
    gu(1)
    ys[0].y5()
    ys[3].y3()
    hg.l1()
    hg.fin()
    ys[1].y5()
    grad_down()
    ys[2].y5()
    ys[3].y5()
    for c in sends:
        c.wait_send()


def put_out(a, b, c, d, ao, bo, co, do, sem):
    copies = [pltpu.make_async_copy(f, t, sem.at[i]) for i, (f, t) in enumerate(((d, do), (b, bo), (c, co), (a, ao)))]
    for c in copies:
        c.start()
    for c in copies:
        c.wait()


def per_device(inputs, cotangent, gate_pre, up_pre, w_gate, w_up, w_down):
    t, d = inputs.shape
    ff = gate_pre.shape[1]
    br = t // NH
    tokens = 16 * t
    scale = 1.0 / math.sqrt(tokens)

    def vm(*shape, kind=BF16):
        return pltpu.VMEM(shape, kind)

    scratch = [
        vm(NH, 2, 8, br, d), vm(NH, 2, 8, br, d), vm(d, tokens), vm(NH, 2, 8, br, ff), vm(NH, 2, 8, br, 2 * ff),
        vm(ff, d), vm(d, 2 * ff), vm(NH, br, ff), vm(NH, br, ff),
        vm(NH, 8, br, ff), vm(NH, 8, br, ff), vm(NH, 8, br, ff, kind=F32),
        vm(NH, 2, br, ff), vm(NH, 2, br, ff), vm(NH, 2, 2, br, ff), vm(NH, 2, 2, br, ff),
        vm(NH, br, ff, kind=F32), vm(NH, br, ff), vm(NH, br, ff),
        vm(NH, 2, 8, br, d, kind=F32),
        vm(NH, 2, 2, br, d), vm(NH, 2, 2, br, d), vm(NH, 2, 2, 2, br, d), vm(NH, 2, 2, 2, br, d),
        vm(NH, 2, 2, br, d, kind=F32),
        vm(NH, 3, br, d), vm(NH, 3, br, d), vm(3, 2, 2, br, d), vm(3, 2, 2, br, d),
        pltpu.SemaphoreType.DMA((N_SEM,)), pltpu.SemaphoreType.DMA((N_SEM,)), pltpu.SemaphoreType.DMA((16,)),
    ]
    hbm = pl.BlockSpec(memory_space=pl.ANY)
    gi, gg, gup, gd = pl.pallas_call(
        functools.partial(kernel, scale),
        out_shape=(
            pltpu.VMEM((NH, br, d), BF16), pltpu.VMEM((d, ff), F32), pltpu.VMEM((d, ff), F32), pltpu.VMEM((ff, d), F32),
        ),
        in_specs=[hbm] * 7,
        out_specs=(pl.BlockSpec(memory_space=pltpu.VMEM),) * 4,
        scratch_shapes=scratch,
        compiler_params=pltpu.CompilerParams(
            collective_id=0, has_side_effects=True, vmem_limit_bytes=VMEM_LIMIT
        ),
    )(
        inputs.reshape(NH, br, d), cotangent.reshape(NH, br, d), gate_pre.reshape(NH, br, ff),
        up_pre.reshape(NH, br, ff), w_gate, w_up, w_down,
    )
    vmem = pl.BlockSpec(memory_space=pltpu.VMEM)
    gi, gg, gup, gd = pl.pallas_call(
        put_out,
        out_shape=(
            jax.ShapeDtypeStruct((NH, br, d), BF16),
            jax.ShapeDtypeStruct((d, ff), F32),
            jax.ShapeDtypeStruct((d, ff), F32),
            jax.ShapeDtypeStruct((ff, d), F32),
        ),
        in_specs=[vmem] * 4,
        out_specs=(hbm,) * 4,
        scratch_shapes=[pltpu.SemaphoreType.DMA((4,))],
        compiler_params=pltpu.CompilerParams(vmem_limit_bytes=1024 * 1024),
    )(gi, gg, gup, gd)
    return gi.reshape(t, d), gg, gup, gd


def solution(mesh):
    split = Mesh(mesh.devices.reshape(2, 4, 2, 4, 4), ROW + COL)
    in_specs = (P(COL, ROW), P(COL, ROW), P(ROW, COL), P(ROW, COL), P(ROW, COL), P(ROW, COL), P(COL, ROW))
    out_specs = (P(COL, ROW), P(ROW, COL), P(ROW, COL), P(COL, ROW))
    return jax.shard_map(per_device, mesh=split, in_specs=in_specs, out_specs=out_specs, check_vma=False)
```

```python
import functools
import math

import jax
import jax.numpy as jnp
from jax import lax
from jax.experimental import pallas as pl
from jax.experimental.pallas import tpu as pltpu
from jax.sharding import Mesh
from jax.sharding import PartitionSpec as P

ROW = ("zl", "x", "core")
COL = ("y", "zh")
SIZES = {"zl": 2, "x": 4, "core": 2, "y": 4, "zh": 4}
MESH = pl.DeviceIdType.MESH
F32, BF16 = jnp.float32, jnp.bfloat16
NH = 4
RG_MODE = ('A', 'A', 'A', 'A')
HG_MODE = '0'
CG_DIRECT = (0,)
Y_DIRECT = (3,)
N_SEM = 320
VMEM_LIMIT = 50 * 1024 * 1024
TN = 512


def nt(left, right):
    return lax.dot_general(left, right, (((1,), (1,)), ((), ())), preferred_element_type=F32)


def kernel(
    scale,
    inp_hbm, cot_hbm, gate_hbm, up_hbm, wg_hbm, wu_hbm, wd_hbm,
    OGI, OGG, OGU, OD,
    CT, IN, INT, HID, GU, WD, WGU, GATE, UP,
    PC, RC, S, XA, XAR, XB, XBR, R, ZS, ZR,
    GIP, YA, YAR, YB, YBR, R2, HB, HBR, YD, YDR,
    ssem, rsem, lsem,
):
    at = {a: lax.axis_index(a) for a in SIZES}
    x, y, zh, zl, k = at["x"], at["y"], at["zh"], at["zl"], at["core"]
    br = CT.shape[3]

    def step(axis, d):
        return lax.rem(at[axis] + (d + SIZES[axis]), SIZES[axis])

    def peer(axis, d):
        return {axis: step(axis, d)}

    sends = []

    def send(src, dst, to):
        i = len(sends)
        c = pltpu.make_async_remote_copy(
            src_ref=src, dst_ref=dst, send_sem=ssem.at[i], recv_sem=rsem.at[i],
            device_id=to, device_id_type=MESH,
        )
        c.start()
        sends.append(c)
        return c

    n_local = [0]

    def local(src, dst):
        c = pltpu.make_async_copy(src, dst, lsem.at[n_local[0]])
        n_local[0] += 1
        c.start()
        return c

    ck, cb = lax.rem(zh, 2), 2 * y + zh // 2

    barrier = pltpu.get_barrier_semaphore()
    peers = [peer("x", 1), peer("x", -1), peer("y", 1), peer("y", -1), peer("zh", 1), peer("zh", -1),
             peer("y", 2), peer("zh", 2), peer("zl", 1), peer("core", 1)]
    for p in peers:
        pl.semaphore_signal(barrier, inc=1, device_id=p, device_id_type=MESH)

    own_cot = local(cot_hbm, CT.at[:, ck, cb])
    load_gate = local(gate_hbm, GATE)
    load_up = local(up_hbm, UP)
    load_wd = local(wd_hbm, WD)
    own_inp = local(inp_hbm, IN.at[:, ck, cb])
    load_wg = local(wg_hbm, WGU.at[:, pl.ds(0, 1024)])
    load_wu = local(wu_hbm, WGU.at[:, pl.ds(1024, 1024)])

    pl.semaphore_wait(barrier, len(peers))

    class ColGather:
        def __init__(self, block, halves, direct=False):
            self.block, self.halves, self.direct = block, halves, direct
            self.y, self.f = {}, {}

        def at(self, dy, dz):
            yy, zz = step("y", dy), step("zh", dz)
            return self.block(lax.rem(zz, 2), 2 * yy + zz // 2)

        def ysend(self, dz):
            b = self.at(0, dz)
            self.y[dz] = (send(b, b, peer("y", 1)), send(b, b, peer("y", -1)))
            if self.direct:
                self.f[dz] = send(b, b, peer("y", 2))

        def sz(self):
            b = self.at(0, 0)
            self.z1 = (send(b, b, peer("zh", 1)), send(b, b, peer("zh", -1)))
            if self.direct:
                self.z2p = send(b, b, peer("zh", 2))

        def sy(self):
            self.ysend(0)

        def zfp(self):
            self.z1[0].wait_recv()
            if self.direct:
                return
            b = self.halves(self.at(0, -1))[0]
            self.z2p = send(b, b, peer("zh", 1))

        def zfm(self):
            self.z1[1].wait_recv()
            if self.direct:
                return
            b = self.halves(self.at(0, 1))[1]
            self.z2m = send(b, b, peer("zh", -1))

        def ys(self, dz):
            self.ysend(dz)

        def zl(self):
            self.z2p.wait_recv()
            if not self.direct:
                self.z2m.wait_recv()
            self.ysend(2)

        def yfp(self, dz):
            self.y[dz][0].wait_recv()
            b = self.at(-1, dz)
            self.f[dz] = send(b, b, peer("y", 1))

        def yfm(self, dz):
            self.y[dz][1].wait_recv()
            b = self.at(1, dz)
            self.f[dz] = send(b, b, peer("y", -1))

        def fin(self):
            for dz in self.y:
                if self.direct or dz in (0, 2):
                    self.y[dz][1].wait_recv()
                if self.direct or dz in (1, -1):
                    self.y[dz][0].wait_recv()
            for c in self.f.values():
                c.wait_recv()

    def row_halves(ref):
        return ref.at[pl.ds(0, br // 2)], ref.at[pl.ds(br // 2, br // 2)]

    def piece_halves(ref):
        return ref.at[pl.ds(0, NH // 2)], ref.at[pl.ds(NH // 2, NH // 2)]

    cg = [ColGather(lambda q, b, h=h: CT.at[h, q, b], row_halves, h in CG_DIRECT) for h in range(NH)]
    cgi = ColGather(lambda q, b: IN.at[:, q, b], piece_halves)

    class RowGather:
        def __init__(self, block, mode, mirror):
            self.block, self.mode, self.mirror = block, mode, mirror
            self.core = []

        def at(self, dx, dzl):
            return self.block(k, step("zl", dzl) * 4 + step("x", dx))

        def to(self, dx, dzl, axis, d=1):
            b = self.at(dx, dzl)
            return send(b, b, peer(axis, d))

        def share(self, dx, dzl):
            self.core.append(self.to(dx, dzl, "core"))

        def sz(self):
            self.z = self.to(0, 0, "zl")

        def sx(self):
            self.x0 = (self.to(0, 0, "x", 1), self.to(0, 0, "x", -1))

        def sc(self):
            self.share(0, 0)

        def f0p(self):
            self.x0[0].wait_recv()
            if not self.mirror:
                self.f0 = self.to(-1, 0, "x", 1)

        def s10(self):
            self.share(-1, 0)

        def f0m(self):
            self.x0[1].wait_recv()
            if self.mirror:
                self.f0 = self.to(1, 0, "x", -1)
            self.share(1, 0)

        def l0(self):
            self.f0.wait_recv()
            self.share(2, 0)

        def zx(self):
            self.z.wait_recv()
            up = self.to(0, 1, "x", 1) if self.mode != "B" else None
            self.x1 = (up, self.to(0, 1, "x", -1))

        def zc(self):
            self.share(0, 1)

        def zp(self):
            self.z1 = self.to(-1, 0, "zl")

        def z2(self):
            self.f1 = self.to(2, 0, "zl")

        def f1p(self):
            (self.z1 if self.mode == "B" else self.x1[0]).wait_recv()
            self.share(-1, 1)

        def f1m(self):
            self.x1[1].wait_recv()
            if self.mode == "0":
                self.f1 = self.to(1, 1, "x", -1)
            self.share(1, 1)

        def l1(self):
            self.f1.wait_recv()
            self.share(2, 1)

        def fin(self):
            for c in self.core:
                c.wait_recv()

    hg = RowGather(lambda q, b: HID.at[:, q, b], HG_MODE, False)
    rg = [RowGather(lambda q, b, h=h: GU.at[h, q, b], RG_MODE[h], RG_MODE[h] == "A" and h % 2 == 1) for h in range(NH)]

    ready = []

    def when(*copies):
        for c in copies:
            if id(c) not in ready:
                ready.append(id(c))
                c.wait()

    def hidden():
        when(load_gate, load_up)

        @pl.loop(0, NH * br // 32)
        def _(i):
            h, s = i // (br // 32), pl.multiple_of(lax.rem(i, br // 32) * 32, 32)
            g = GATE[h, pl.ds(s, 32)].astype(F32)
            u = UP[h, pl.ds(s, 32)].astype(F32)
            HID[h, k, zl * 4 + x, pl.ds(s, 32)] = (g * jax.nn.sigmoid(g) * u).astype(BF16)

    core_part = {}

    def gho(h):
        when(load_wd)

        @pl.loop(0, 1024 // TN)
        def _(n):
            c = pl.multiple_of(n * TN, TN)
            a = CT[h, 1 - k].reshape(8 * br, CT.shape[4])
            p = nt(a, WD[pl.ds(c, TN), :])
            PC[h, :, :, pl.ds(c, TN)] = p.astype(PC.dtype).reshape(8, br, TN)

        core_part[h] = send(PC.at[h], RC.at[h], peer("core", 1))

    def ghw(h):
        @pl.loop(0, 1024 // TN)
        def _(n):
            c = pl.multiple_of(n * TN, TN)
            a = CT[h, k].reshape(8 * br, CT.shape[4])
            S[h, :, :, pl.ds(c, TN)] = nt(a, WD[pl.ds(c, TN), :]).reshape(8, br, TN)

    class XScatter:
        def __init__(self, h):
            self.h = h

        def part(self, dx, z):
            return z * 4 + step("x", dx)

        def total(self, b):
            return S[self.h, b] + RC[self.h, b].astype(F32)

        def x1a(self):
            h = self.h
            core_part[h].wait_recv()
            for z in range(2):
                XA[h, z] = self.total(self.part(2, z)).astype(BF16)
            self.a = (send(XA.at[h, 0], XAR.at[h, 0], peer("x", 1)), send(XA.at[h, 1], XAR.at[h, 1], peer("x", -1)))

        def x1c(self):
            h = self.h
            XB[h, 0, 1] = self.total(self.part(1, 1)).astype(BF16)
            XB[h, 1, 0] = self.total(self.part(-1, 0)).astype(BF16)
            self.b1 = (send(XB.at[h, 0, 1], XBR.at[h, 0, 1], peer("x", 1)),
                       send(XB.at[h, 1, 0], XBR.at[h, 1, 0], peer("x", -1)))

        def x1b(self):
            for b in (self.part(1, 0), self.part(-1, 1), self.part(0, 0), self.part(0, 1)):
                S[self.h, b] = self.total(b)

        def x2p(self):
            h = self.h
            self.a[0].wait_recv()
            XB[h, 0, 0] = (S[h, self.part(1, 0)] + XAR[h, 0].astype(F32)).astype(BF16)
            self.b2p = send(XB.at[h, 0, 0], XBR.at[h, 0, 0], peer("x", 1))

        def x2m(self):
            h = self.h
            self.a[1].wait_recv()
            XB[h, 1, 1] = (S[h, self.part(-1, 1)] + XAR[h, 1].astype(F32)).astype(BF16)
            self.b2m = send(XB.at[h, 1, 1], XBR.at[h, 1, 1], peer("x", -1))

        def x3(self):
            h = self.h
            for c in self.b1 + (self.b2p, self.b2m):
                c.wait_recv()

            def total(z):
                return S[h, self.part(0, z)] + XBR[h, 0, z].astype(F32) + XBR[h, 1, z].astype(F32)

            ZS[h] = total(1 - zl).astype(ZS.dtype)
            self.z = send(ZS.at[h], ZR.at[h], peer("zl", 1))
            R[h] = total(zl)

        def grads(self):
            h = self.h
            self.z.wait_recv()

            @pl.loop(0, br // 16)
            def _(i):
                s = pl.multiple_of(i * 16, 16)
                gh = R[h, pl.ds(s, 16)] + ZR[h, pl.ds(s, 16)].astype(F32)
                g = GATE[h, pl.ds(s, 16)].astype(F32)
                u = UP[h, pl.ds(s, 16)].astype(F32)
                sig = jax.nn.sigmoid(g)
                b = zl * 4 + x
                GU[h, k, b, pl.ds(s, 16), pl.ds(0, 1024)] = (gh * u * sig * (1.0 + g * (1.0 - sig))).astype(BF16)
                GU[h, k, b, pl.ds(s, 16), pl.ds(1024, 1024)] = (gh * (g * sig)).astype(BF16)

    xs = [XScatter(h) for h in range(NH)]

    def gi(h):
        when(load_wg, load_wu)

        @pl.loop(0, 2)
        def _(q):
            @pl.loop(0, 512 // TN)
            def _(i):
                c = pl.multiple_of(i * TN, TN)
                a = GU[h, q].reshape(8 * br, GU.shape[4])
                GIP[h, q, :, :, pl.ds(c, TN)] = nt(a, WGU[pl.ds(c, TN), :]).reshape(8, br, TN)

    class YScatter:
        def __init__(self, h):
            self.h = h

        def part(self, dy, q):
            return GIP[self.h, q, pl.ds(2 * step("y", dy), 2)]

        def y1(self):
            h = self.h
            if h in Y_DIRECT:
                self.d = []
                for i, dy in enumerate((2, 1, -1)):
                    for q in range(2):
                        YD[i, q] = self.part(dy, q).astype(BF16)
                    self.d.append(send(YD.at[i], YDR.at[i], peer("y", dy)))
                return
            for q in range(2):
                YA[h, q] = self.part(2, q).astype(BF16)
            self.a = (send(YA.at[h, 0], YAR.at[h, 0], peer("y", 1)), send(YA.at[h, 1], YAR.at[h, 1], peer("y", -1)))

        def y1b(self):
            h = self.h
            YB[h, 0, 1] = self.part(1, 1).astype(BF16)
            YB[h, 1, 0] = self.part(-1, 0).astype(BF16)
            self.b1 = (send(YB.at[h, 0, 1], YBR.at[h, 0, 1], peer("y", 1)),
                       send(YB.at[h, 1, 0], YBR.at[h, 1, 0], peer("y", -1)))

        def y2p(self):
            h = self.h
            self.a[0].wait_recv()
            YB[h, 0, 0] = (self.part(1, 0) + YAR[h, 0].astype(F32)).astype(BF16)
            self.b2p = send(YB.at[h, 0, 0], YBR.at[h, 0, 0], peer("y", 1))

        def y2m(self):
            h = self.h
            self.a[1].wait_recv()
            YB[h, 1, 1] = (self.part(-1, 1) + YAR[h, 1].astype(F32)).astype(BF16)
            self.b2m = send(YB.at[h, 1, 1], YBR.at[h, 1, 1], peer("y", -1))

        def y3(self):
            h = self.h
            if h in Y_DIRECT:
                for c in self.d:
                    c.wait_recv()
                for q in range(2):
                    R2[h, q] = (self.part(0, q) + YDR[1, q].astype(F32)) + (YDR[2, q].astype(F32) + YDR[0, q].astype(F32))
            else:
              for c in self.b1 + (self.b2p, self.b2m):
                c.wait_recv()
              for q in range(2):
                R2[h, q] = self.part(0, q) + YBR[h, 0, q].astype(F32) + YBR[h, 1, q].astype(F32)

            def zpart(dz):
                zz = step("zh", dz)
                return R2[h, lax.rem(zz, 2), zz // 2]

            self.zpart = zpart
            self.zs = []
            for i, dz in enumerate((2, 1, -1)):
                HB[h, i] = zpart(dz).astype(BF16)
                self.zs.append(send(HB.at[h, i], HBR.at[h, i], peer("zh", dz)))

        def y5(self):
            h = self.h
            for c in self.zs:
                c.wait_recv()
            OGI[h] = (
                (self.zpart(0) + HBR[h, 1].astype(F32)) + (HBR[h, 2].astype(F32) + HBR[h, 0].astype(F32))
            ).astype(BF16)

    ys = [YScatter(h) for h in range(NH)]

    def transpose_inputs():
        @pl.loop(0, NH * 2)
        def _(i):
            rows = 8 * br
            v = IN[i // 2, lax.rem(i, 2)].reshape(rows, IN.shape[4])
            INT[:, pl.ds(pl.multiple_of(i * rows, rows), rows)] = v.T

    def grad_down():
        @pl.loop(0, 4)
        def _(i):
            c = pl.multiple_of(i * 256, 256)
            a = HID[:, :, :, :, pl.ds(c, 256)].reshape(NH * 16 * br, 256)
            b = CT[...].reshape(NH * 16 * br, CT.shape[4])
            p = lax.dot_general(a, b, (((0,), (0,)), ((), ())), preferred_element_type=F32)
            OD[pl.ds(c, 256), :] = p * scale

    added = []

    def gu(h):
        rows = 16 * br
        first, last = not added, len(added) == NH - 1
        added.append(h)

        for out, base in ((OGG, 0), (OGU, 1024)):
            @pl.loop(0, 4)
            def _(i):
                c = pl.multiple_of(i * 256, 256)
                from_gu = pl.ds(pl.multiple_of(base + i * 256, 256), 256)
                p = jnp.dot(INT[:, pl.ds(h * rows, rows)], GU[h, :, :, :, from_gu].reshape(rows, 256),
                            preferred_element_type=F32)
                if not first:
                    p = p + out[:, pl.ds(c, 256)]
                out[:, pl.ds(c, 256)] = p * scale if last else p

    own_cot.wait()
    cg[1].sz()
    cg[0].sz()
    cg[1].sy()
    hidden()
    cg[2].sz()
    cg[2].sy()
    cg[3].sy()
    hg.sx()
    cg[0].sy()
    hg.sc()
    cg[1].yfp(0)
    cg[1].zfp()
    cg[1].ys(-1)
    cg[1].zfm()
    cg[1].ys(1)
    cg[3].sz()
    cg[0].zfp()
    cg[0].ys(-1)
    cg[0].zfm()
    cg[0].ys(1)
    cg[0].zl()
    cg[2].zfm()
    cg[2].zfp()
    cg[1].yfm(1)
    cg[1].zl()
    cg[2].yfp(0)
    hg.f0p()
    cg[2].ys(-1)
    cg[2].ys(1)
    cg[3].zfp()
    cg[3].zfm()
    cg[1].yfm(-1)
    cg[1].yfp(2)
    own_inp.wait()
    cgi.sz()
    cg[2].zl()
    cg[0].fin()
    gho(0)
    cg[3].ys(1)
    cg[3].ys(-1)
    hg.s10()
    cg[3].zl()
    hg.sz()
    cg[2].yfm(-1)
    ghw(0)
    xs[0].x1a()
    xs[0].x1c()
    cg[3].yfp(0)
    cg[2].yfm(1)
    cg[1].fin()
    gho(1)
    cg[2].yfp(2)
    cg[3].yfm(1)
    ghw(1)
    cg[3].yfm(-1)
    xs[1].x1a()
    xs[0].x1b()
    xs[1].x1c()
    xs[0].x2p()
    cg[3].yfp(2)
    xs[0].x2m()
    cg[2].fin()
    gho(2)
    ghw(2)
    cgi.zfm()
    cgi.ys(1)
    cgi.zfp()
    cgi.ys(-1)
    xs[2].x1a()
    hg.l0()
    cgi.sy()
    xs[1].x1b()
    xs[1].x2p()
    xs[1].x2m()
    cg[3].fin()
    xs[2].x1c()
    gho(3)
    xs[0].x3()
    xs[2].x1b()
    ghw(3)
    xs[3].x1a()
    xs[2].x2p()
    xs[2].x2m()
    xs[3].x1c()
    xs[1].x3()
    xs[0].grads()
    cgi.yfm(-1)
    rg[0].sx()
    rg[0].sc()
    rg[0].sz()
    xs[2].x3()
    xs[3].x1b()
    xs[3].x2p()
    xs[1].grads()
    rg[1].sz()
    rg[1].sx()
    cgi.zl()
    rg[1].sc()
    xs[3].x2m()
    rg[0].f0p()
    xs[2].grads()
    cgi.yfp(0)
    rg[2].sx()
    rg[2].sz()
    rg[1].f0m()
    rg[0].zx()
    rg[2].sc()
    xs[3].x3()
    rg[0].f0m()
    rg[1].zx()
    rg[1].zc()
    rg[0].l0()
    hg.f0m()
    rg[0].z2()
    xs[3].grads()
    rg[3].sc()
    rg[1].f0p()
    cgi.yfp(2)
    cgi.yfm(1)
    rg[2].f0p()
    rg[3].sx()
    rg[2].s10()
    rg[1].l0()
    rg[1].z2()
    rg[0].zc()
    rg[1].s10()
    rg[2].zx()
    rg[2].zc()
    rg[0].s10()
    rg[0].f1p()
    rg[3].sz()
    rg[0].f1m()
    rg[0].l1()
    rg[0].fin()
    gi(0)
    ys[0].y1()
    ys[0].y1b()
    rg[1].f1m()
    rg[2].f0m()
    rg[1].f1p()
    cgi.fin()
    transpose_inputs()
    rg[1].l1()
    rg[2].l0()
    rg[2].z2()
    rg[3].f0m()
    gu(0)
    rg[3].zx()
    ys[0].y2p()
    rg[2].f1m()
    rg[3].f0p()
    rg[1].fin()
    ys[0].y2m()
    gi(1)
    ys[1].y1()
    rg[2].l1()
    rg[2].f1p()
    rg[3].s10()
    rg[3].l0()
    rg[3].z2()
    ys[1].y1b()
    rg[3].zc()
    hg.zx()
    hg.zc()
    rg[2].fin()
    gi(2)
    ys[2].y1()
    rg[3].f1p()
    ys[2].y1b()
    rg[3].f1m()
    gu(2)
    rg[3].l1()
    ys[1].y2p()
    ys[1].y2m()
    ys[0].y3()
    ys[2].y2p()
    ys[2].y2m()
    rg[3].fin()
    gi(3)
    ys[3].y1()
    hg.f1m()
    hg.f1p()
    ys[1].y3()
    gu(3)
    ys[2].y3()
    gu(1)
    ys[0].y5()
    ys[3].y3()
    hg.l1()
    hg.fin()
    ys[1].y5()
    grad_down()
    ys[2].y5()
    ys[3].y5()
    for c in sends:
        c.wait_send()


def put_out(a, b, c, d, ao, bo, co, do, sem):
    copies = [pltpu.make_async_copy(f, t, sem.at[i]) for i, (f, t) in enumerate(((d, do), (b, bo), (c, co), (a, ao)))]
    for c in copies:
        c.start()
    for c in copies:
        c.wait()


def per_device(inputs, cotangent, gate_pre, up_pre, w_gate, w_up, w_down):
    t, d = inputs.shape
    ff = gate_pre.shape[1]
    br = t // NH
    tokens = 16 * t
    scale = 1.0 / math.sqrt(tokens)

    def vm(*shape, kind=BF16):
        return pltpu.VMEM(shape, kind)

    scratch = [
        vm(NH, 2, 8, br, d), vm(NH, 2, 8, br, d), vm(d, tokens), vm(NH, 2, 8, br, ff), vm(NH, 2, 8, br, 2 * ff),
        vm(ff, d), vm(d, 2 * ff), vm(NH, br, ff), vm(NH, br, ff),
        vm(NH, 8, br, ff), vm(NH, 8, br, ff), vm(NH, 8, br, ff, kind=F32),
        vm(NH, 2, br, ff), vm(NH, 2, br, ff), vm(NH, 2, 2, br, ff), vm(NH, 2, 2, br, ff),
        vm(NH, br, ff, kind=F32), vm(NH, br, ff), vm(NH, br, ff),
        vm(NH, 2, 8, br, d, kind=F32),
        vm(NH, 2, 2, br, d), vm(NH, 2, 2, br, d), vm(NH, 2, 2, 2, br, d), vm(NH, 2, 2, 2, br, d),
        vm(NH, 2, 2, br, d, kind=F32),
        vm(NH, 3, br, d), vm(NH, 3, br, d), vm(3, 2, 2, br, d), vm(3, 2, 2, br, d),
        pltpu.SemaphoreType.DMA((N_SEM,)), pltpu.SemaphoreType.DMA((N_SEM,)), pltpu.SemaphoreType.DMA((16,)),
    ]
    hbm = pl.BlockSpec(memory_space=pl.ANY)
    gi, gg, gup, gd = pl.pallas_call(
        functools.partial(kernel, scale),
        out_shape=(
            pltpu.VMEM((NH, br, d), BF16), pltpu.VMEM((d, ff), F32), pltpu.VMEM((d, ff), F32), pltpu.VMEM((ff, d), F32),
        ),
        in_specs=[hbm] * 7,
        out_specs=(pl.BlockSpec(memory_space=pltpu.VMEM),) * 4,
        scratch_shapes=scratch,
        compiler_params=pltpu.CompilerParams(
            collective_id=0, has_side_effects=True, vmem_limit_bytes=VMEM_LIMIT
        ),
    )(
        inputs.reshape(NH, br, d), cotangent.reshape(NH, br, d), gate_pre.reshape(NH, br, ff),
        up_pre.reshape(NH, br, ff), w_gate, w_up, w_down,
    )
    vmem = pl.BlockSpec(memory_space=pltpu.VMEM)
    gi, gg, gup, gd = pl.pallas_call(
        put_out,
        out_shape=(
            jax.ShapeDtypeStruct((NH, br, d), BF16),
            jax.ShapeDtypeStruct((d, ff), F32),
            jax.ShapeDtypeStruct((d, ff), F32),
            jax.ShapeDtypeStruct((ff, d), F32),
        ),
        in_specs=[vmem] * 4,
        out_specs=(hbm,) * 4,
        scratch_shapes=[pltpu.SemaphoreType.DMA((4,))],
        compiler_params=pltpu.CompilerParams(vmem_limit_bytes=1024 * 1024),
    )(gi, gg, gup, gd)
    return gi.reshape(t, d), gg, gup, gd


def solution(mesh):
    split = Mesh(mesh.devices.reshape(2, 4, 2, 4, 4), ROW + COL)
    in_specs = (P(COL, ROW), P(COL, ROW), P(ROW, COL), P(ROW, COL), P(ROW, COL), P(ROW, COL), P(COL, ROW))
    out_specs = (P(COL, ROW), P(ROW, COL), P(ROW, COL), P(COL, ROW))
    return jax.shard_map(per_device, mesh=split, in_specs=in_specs, out_specs=out_specs, check_vma=False)
```
